256 devices in a mesh: shot: 8 (over x_hi, y), rcv: 32 (over x_lo, z, core).
Axes of the slice: x: 4 (x_hi: 2, x_lo: 2; x = x_hi * 2 + x_lo), y: 4, z: 8, core: 2. Of those that a mesh axis runs over, the one named last changes fastest.
Arguments:
- modeled: bfloat16 [2, 64, 8, 256, 512], P(None, 'shot', None, 'rcv'), may hold values from -9 to 9
- observed: bfloat16 [2, 8, 64, 256, 512], P(None, 'shot', 'rcv'), may hold values from -60 to 60
- mask: int32 [64, 8, 256], P('shot', None, 'rcv'), may hold values 0 or 1
- shot_order: int32 [64], replicated, may hold values from 0 to 63, as said below
- line_of_slot: int32 [8], replicated, may hold values from 0 to 7, as said below
- coupling: bfloat16 [2, 512, 512], replicated, may hold values from -0.25 to 0.25
- wavelet: float32 [2, 512], replicated, may hold values from -4 to 4
- damping: float32 [512], replicated, may hold values from 32768 to 524288
Outputs:
- new_wavelet: float32 [2, 512], replicated
- residual_out: bfloat16 [2, 64, 8, 256, 512], P(None, 'shot', None, 'rcv')
The draws below stay inside these ranges and needn't reach their ends.
Inputs may be any that keep to these rules, and one draw needn't show every extreme that they name: Group g holds the shots shot_order[g * 8] to shot_order[(g + 1) * 8 - 1]; each shot number appears once. `line_of_slot`: each line appears in exactly one slot.
All inputs are finite; a program needn't handle non-finite values. No bound on the sum of `mask` on one device may be relied on, other than what follows from the above.
Results may differ from the reference program's by a relative error of at most 0.00045.
Values may be sent and summed in bfloat16 or wider, within the bound.
No kernel may reach another device: no remote copies, remote signals or barrier semaphores. Data moves between devices by JAX's collectives and lax.ppermute only.
A program may use at most 64 MiB of HBM per device.

```python
import math
import jax
import jax.numpy as jnp
from jax import lax

SG = 8
RB = 8
F = 512
LINES = 8
SHOTS = 64
LINE_R = 256


def build_survey(key):
    base = jax.random.fold_in(key, 811)
    order = jax.random.permutation(jax.random.fold_in(base, 1), SHOTS).astype(jnp.int32)
    slots = jax.random.permutation(jax.random.fold_in(base, 2), LINES).astype(jnp.int32)
    shape = (2, SHOTS, LINES, LINE_R, F)
    traces = jnp.clip(jax.random.normal(jax.random.fold_in(base, 3), shape, jnp.float32), -6.0, 6.0)
    noise_level = 0.3
    traces = traces.astype(jnp.bfloat16).astype(jnp.float32)
    source = jnp.clip(jax.random.normal(jax.random.fold_in(base, 4), (2, F), jnp.float32), -4.0, 4.0)
    group_pos = (jnp.arange(SHOTS) // SG).astype(jnp.float32) / (SHOTS // SG - 1)
    piece_pos = (jnp.arange(LINE_R) // RB).astype(jnp.float32) / (LINE_R // RB - 1)
    amplitude = (3.0 ** group_pos)[:, None, None, None] * (3.0 ** piece_pos)[None, None, :, None] / 3.0
    src_re = source[0][None, None, None, :]
    src_im = source[1][None, None, None, :]
    clean_re = amplitude * (src_re * traces[0] - src_im * traces[1])
    clean_im = amplitude * (src_re * traces[1] + src_im * traces[0])
    noise = jax.random.normal(jax.random.fold_in(base, 6), shape, jnp.float32) * noise_level
    grouped = jnp.stack([clean_re, clean_im]) + noise
    natural = jnp.zeros(shape, jnp.float32).at[:, order].set(grouped)
    by_slot = jnp.take(natural, slots, axis=2)
    stored = jnp.clip(jnp.transpose(by_slot, (0, 2, 1, 3, 4)), -60.0, 60.0)
    return (traces, stored)


def draw_modeled(key, part):
    return build_survey(key)[0].astype(jnp.bfloat16)


def draw_observed(key, part):
    return build_survey(key)[1].astype(jnp.bfloat16)


def draw_shot_order(key, part):
    base = jax.random.fold_in(key, 811)
    return jax.random.permutation(jax.random.fold_in(base, 1), SHOTS).astype(jnp.int32)


def draw_line_of_slot(key, part):
    base = jax.random.fold_in(key, 811)
    return jax.random.permutation(jax.random.fold_in(base, 2), LINES).astype(jnp.int32)


def place_ends(drawn, stream_key, least, largest):
    dims = drawn.shape
    place = [jax.random.randint(jax.random.fold_in(stream_key, axis), (), 0, dims[axis]) for axis in range(len(dims))]
    drawn = drawn.at[tuple(place)].set(least)
    longest = dims.index(max(dims))
    place[longest] = (place[longest] + 1) % dims[longest]
    return drawn.at[tuple(place)].set(largest)


def centred(stream_key, dims, scale, most, held_as=jnp.bfloat16):
    return jnp.clip(scale * jax.random.normal(stream_key, dims, jnp.float32), -most, most).astype(held_as)


def setup_inputs(seed: int = 0) -> dict:
    arg_keys = jax.random.split(jax.random.key(seed), 9)
    modeled = draw_modeled(jax.random.fold_in(arg_keys[8], 71), 0)
    observed = draw_observed(jax.random.fold_in(arg_keys[8], 71), 0)
    mask = place_ends((jax.random.randint(arg_keys[2], (SHOTS, LINES, LINE_R), 0, 5) < 4).astype(jnp.int32), jax.random.fold_in(arg_keys[2], 1), 0, 1)
    shot_order = draw_shot_order(jax.random.fold_in(arg_keys[8], 71), 0)
    line_of_slot = draw_line_of_slot(jax.random.fold_in(arg_keys[8], 71), 0)
    coupling = centred(arg_keys[5], (2, F, F), F ** -0.5, 0.25)
    wavelet = centred(arg_keys[6], (2, F), 1.0, 4.0, jnp.float32)
    damping = jnp.clip(jnp.exp(jax.random.uniform(arg_keys[7], (F,), jnp.float32, math.log(32768.0), math.log(524288.0))), 32768.0, 524288.0)
    return {"modeled": modeled, "observed": observed, "mask": mask, "shot_order": shot_order, "line_of_slot": line_of_slot, "coupling": coupling, "wavelet": wavelet, "damping": damping}


def weigh(trace, coupling):
    real_part = jnp.dot(trace[0], coupling[0], preferred_element_type=jnp.float32) - jnp.dot(trace[1], coupling[1], preferred_element_type=jnp.float32)
    imag_part = jnp.dot(trace[0], coupling[1], preferred_element_type=jnp.float32) + jnp.dot(trace[1], coupling[0], preferred_element_type=jnp.float32)
    return real_part, imag_part


def reference(modeled, observed, mask, shot_order, line_of_slot, coupling, wavelet, damping):
    inverse = jnp.zeros((LINES,), jnp.int32).at[line_of_slot].set(jnp.arange(LINES, dtype=jnp.int32))
    live = mask.astype(jnp.float32)

    def fields(line):
        slot = inverse[line]
        obs_line = lax.dynamic_index_in_dim(observed, slot, 1, keepdims=False)
        obs_line = jnp.take(obs_line, shot_order, axis=1)
        mod_line = lax.dynamic_index_in_dim(modeled, line, 2, keepdims=False)
        live_line = lax.dynamic_index_in_dim(live, line, 1, keepdims=False)[..., None]
        wd_re, wd_im = weigh(obs_line, coupling)
        wg_re, wg_im = weigh(mod_line, coupling)
        return wd_re, wd_im, wg_re, wg_im, live_line

    def partials(line):
        wd_re, wd_im, wg_re, wg_im, live_line = fields(line)
        res_re = live_line * (wd_re - (wavelet[0] * wg_re - wavelet[1] * wg_im))
        res_im = live_line * (wd_im - (wavelet[0] * wg_im + wavelet[1] * wg_re))
        num_re = jnp.sum(wg_re * res_re + wg_im * res_im, axis=(0, 1))
        num_im = jnp.sum(wg_re * res_im - wg_im * res_re, axis=(0, 1))
        den = jnp.sum(live_line * (wg_re * wg_re + wg_im * wg_im), axis=(0, 1))
        return jnp.stack([num_re, num_im]), den

    lines = jnp.arange(LINES, dtype=jnp.int32)
    nums, dens = lax.map(partials, lines)
    num = jnp.sum(nums, axis=0)
    den = jnp.sum(dens, axis=0)
    new_wavelet = wavelet + num / (den + damping)[None, :]

    def outputs(line):
        wd_re, wd_im, wg_re, wg_im, live_line = fields(line)
        out_re = live_line * (wd_re - (new_wavelet[0] * wg_re - new_wavelet[1] * wg_im))
        out_im = live_line * (wd_im - (new_wavelet[0] * wg_im + new_wavelet[1] * wg_re))
        return jnp.stack([out_re, out_im]).astype(jnp.bfloat16)

    stacked = lax.map(outputs, lines)
    residual_out = jnp.transpose(stacked, (1, 2, 0, 3, 4))
    return new_wavelet, residual_out
```

```python
import jax
import jax.numpy as jnp
from jax import lax
from jax.experimental import pallas as pl
from jax.experimental.pallas import tpu as pltpu
from jax.sharding import Mesh, PartitionSpec as P

F32 = jnp.float32
BF16 = jnp.bfloat16
SHOT = ("xh", "y")
RCV = ("xl", "z", "c")
REST = ("xh", "y", "xl")

VM = pl.BlockSpec(memory_space=pltpu.VMEM)
SM = pl.BlockSpec(memory_space=pltpu.SMEM)
ANY = pl.BlockSpec(memory_space=pl.ANY)


def call(body, outs, in_specs, out_specs=None, scratch=(), limit=12 << 20, flops=0, nbytes=1 << 20):
    many = isinstance(outs, (tuple, list))
    return pl.pallas_call(
        body,
        out_shape=outs,
        in_specs=in_specs,
        out_specs=out_specs if out_specs is not None else ([VM] * len(outs) if many else VM),
        scratch_shapes=list(scratch),
        compiler_params=pltpu.CompilerParams(vmem_limit_bytes=limit),
        cost_estimate=pl.CostEstimate(flops=flops, bytes_accessed=nbytes, transcendentals=0),
    )


CHUNKS = 4


def k_spread(obs_ref, out_ref, buf, sem_in, sem_out):
    parts, pieces = obs_ref.shape[:2]
    step = pieces // CHUNKS
    ins, outs = [], []
    for q in range(CHUNKS):
        rows = pl.ds(q * step, step)
        for i in range(parts):
            ins.append(pltpu.make_async_copy(obs_ref.at[i, rows], buf.at[rows, i], sem_in.at[q, i]))
        outs.append(pltpu.make_async_copy(buf.at[rows], out_ref.at[rows], sem_out.at[q]))
    for c in ins:
        c.start()
    for q in range(CHUNKS):
        for i in range(parts):
            ins[q * parts + i].wait()
        outs[q].start()
    for c in outs:
        c.wait()


def k_couple(c_ref, out_ref):
    f = c_ref.shape[1]
    re, im = c_ref[0], c_ref[1]
    out_ref[0, :f] = re
    out_ref[0, f:] = -im
    out_ref[1, :f] = im
    out_ref[1, f:] = re


def k_mask(me_ref, slot_ref, mod_ref, mask_ref, live_ref, *out_refs):
    me = me_ref[0]
    shots, rb = mod_ref.shape[1], mod_ref.shape[3]
    f = mod_ref.shape[4]
    eye = lax.broadcasted_iota(jnp.int32, (rb, rb), 0) == lax.broadcasted_iota(jnp.int32, (rb, rb), 1)
    for b, out_ref in enumerate(out_refs):
        line = slot_ref[lax.bitwise_xor(me, b)]
        for s in range(shots):
            row = mask_ref[s, pl.ds(line, 1)].astype(F32)
            column = jnp.where(eye, row, 0.0).sum(axis=1, keepdims=True)
            rows = pl.ds(s * rb, rb)
            live_ref[b, rows] = jnp.broadcast_to(column, (rb, 128))
            live = jnp.broadcast_to(column, (rb, f)) > 0.5
            for c in range(2):
                x = mod_ref[c, s, line].astype(F32)
                out_ref[c, rows] = jnp.where(live, x, 0.0).astype(BF16)


def window(x, b_ref, d):
    return jnp.dot(x, b_ref[d], preferred_element_type=F32)


def k_window(*refs):
    xs, b_ref, out_ref = refs[:-2], refs[-2], refs[-1]
    x = jnp.concatenate([jnp.concatenate([x[c] for x in xs], axis=0) for c in range(2)], axis=1)
    out_ref[0] = window(x, b_ref, 0)
    out_ref[1] = window(x, b_ref, 1)


def k_window_own(me_ref, own_ref, live_ref, b_ref, out_ref, x_ref):
    me = me_ref[0]
    slots, _, rows, f = own_ref.shape
    for b in range(slots):
        k = lax.bitwise_xor(me, b)
        live = jnp.concatenate([live_ref[b]] * (f // live_ref.shape[2]), axis=1) > 0.5
        for c in range(2):
            x = own_ref[k, c].astype(F32)
            x_ref[b * rows : (b + 1) * rows, c * f : (c + 1) * f] = jnp.where(live, x, 0.0).astype(BF16)
    x = x_ref[...]
    out_ref[0] = window(x, b_ref, 0)
    out_ref[1] = window(x, b_ref, 1)


def k_group(order_ref, own_ref, out_ref):
    groups, _, rows, _ = out_ref.shape
    rb = own_ref.shape[2]
    size = rows // rb
    for g in range(groups):
        for s in range(size):
            n = order_ref[g * size + s]
            j = lax.shift_right_logical(n, 1)
            h = lax.bitwise_and(n, 1)
            for c in range(2):
                out_ref[g, c, s * rb : (s + 1) * rb] = own_ref[j, 2 * c + h]


def fold(x):
    return x.reshape(x.shape[0] // 8, 8, x.shape[1]).sum(axis=0).sum(axis=0, keepdims=True)


def k_cross(me_ref, order_ref, own_ref, b_ref, wg_ref, out_ref, x_ref):
    me = me_ref[0]
    rb, f = own_ref.shape[2:]
    size = order_ref.shape[0] // 8
    for b in range(8):
        g = lax.bitwise_xor(me, b)
        for s in range(size):
            n = order_ref[g * size + s]
            j = lax.shift_right_logical(n, 1)
            h = lax.bitwise_and(n, 1)
            row = (b * size + s) * rb
            for c in range(2):
                x_ref[row : row + rb, c * f : (c + 1) * f] = own_ref[j, 2 * c + h]
    x = x_ref[...]
    wd_re = window(x, b_ref, 0)
    wd_im = window(x, b_ref, 1)
    wg_re, wg_im = wg_ref[0], wg_ref[1]
    out_ref[0:1] = fold(wg_re * wd_re + wg_im * wd_im)
    out_ref[1:2] = fold(wg_re * wd_im - wg_im * wd_re)
    out_ref[2:3] = fold(wg_re * wg_re + wg_im * wg_im)


def k_final(me_ref, slot_ref, wd_ref, wg_ref, sums_ref, wav_ref, damp_ref, nw_ref, out_ref):
    me = me_ref[0]
    total = sums_ref[...].sum(axis=0)
    den = total[2:3]
    wav_re, wav_im = wav_ref[0:1], wav_ref[1:2]
    scale = den + damp_ref[...]
    nw_re = wav_re + (total[0:1] - wav_re * den) / scale
    nw_im = wav_im + (total[1:2] - wav_im * den) / scale
    nw_ref[0:1] = nw_re
    nw_ref[1:2] = nw_im
    _, shots, lines, rb, _ = out_ref.shape
    for b in range(lines):
        line = slot_ref[lax.bitwise_xor(me, b)]
        for s in range(shots):
            rows = pl.ds((b * shots + s) * rb, rb)
            wg_re, wg_im = wg_ref[0, rows], wg_ref[1, rows]
            out_ref[0, s, line] = (wd_ref[0, rows] - (nw_re * wg_re - nw_im * wg_im)).astype(BF16)
            out_ref[1, s, line] = (wd_ref[1, rows] - (nw_re * wg_im + nw_im * wg_re)).astype(BF16)


def swapped(x, axis, bit):
    size = lax.axis_size(axis)
    return lax.ppermute(x, axis, [(i, i ^ bit) for i in range(size)])


def sent_to_all(array, axis):
    size = lax.axis_size(axis)
    return lax.all_to_all(
        jnp.broadcast_to(array[None], (size, *array.shape)), axis, 0, 0, tiled=True
    )


def update(modeled, observed, mask, shot_order, line_of_slot, coupling, wavelet, damping):
    _, shots, lines, rb, f = modeled.shape
    slots = lax.axis_size(SHOT)
    held = observed.shape[2]
    pieces = lax.axis_size(RCV)
    rows = shots * rb
    traces = lines * rows
    flops = 8 * traces * f * f
    me = lax.axis_index(SHOT).astype(jnp.int32).reshape(1)

    own_spread = call(
        k_spread, jax.ShapeDtypeStruct((pieces, 2 * held, rb, f), BF16), [ANY], ANY,
        limit=60 << 20,
        scratch=[
            pltpu.VMEM((pieces, 2 * held, rb, f), BF16),
            pltpu.SemaphoreType.DMA((CHUNKS, 2 * held)),
            pltpu.SemaphoreType.DMA((CHUNKS,)),
        ],
    )(observed.reshape(2 * held, pieces, rb, f))
    own_natural = lax.all_to_all(own_spread, RCV, 0, 0, tiled=True)

    both = call(k_couple, jax.ShapeDtypeStruct((2, 2 * f, f), BF16), [VM])(coupling)
    piece = jax.ShapeDtypeStruct((2, rows, f), BF16)
    live, *masked = call(
        k_mask, (jax.ShapeDtypeStruct((slots, rows, 128), F32), *[piece] * slots),
        [SM, SM, VM, VM],
    )(me, line_of_slot, modeled, mask)
    wide = jax.ShapeDtypeStruct((2, traces, f), F32)
    arrived = [masked[0]]
    for b in range(1, slots):
        arrived.append(swapped(masked[b], SHOT, b))
    wg_here = call(k_window, wide, [VM] * (slots + 1), flops=flops)(*masked, both)
    wg_slot = call(k_window, wide, [VM] * (slots + 1), flops=flops)(*arrived, both)

    own_group = call(
        k_group, jax.ShapeDtypeStruct((slots, 2, rows, f), BF16), [SM, VM],
    )(shot_order, own_natural)
    own_here = lax.all_to_all(own_group, SHOT, 0, 0, tiled=True)
    sums = call(
        k_cross, jax.ShapeDtypeStruct((3, f), F32), [SM, SM, VM, VM, VM],
        scratch=[pltpu.VMEM((traces, 2 * f), BF16)], flops=flops,
    )(me, shot_order, own_natural, both, wg_slot)
    sums = sums.reshape(3 * f // 128, 128)
    for axis, bit in (("c", 1), ("z", 1), ("z", 2), ("z", 4)):
        sums = sums + swapped(sums, axis, bit)
    parts = sent_to_all(sums.reshape(1, 3 * f), REST).reshape(-1, 3, f)
    wd_here = call(
        k_window_own, wide, [SM, VM, VM, VM], flops=flops,
        scratch=[pltpu.VMEM((traces, 2 * f), BF16)],
    )(me, own_here, live, both)

    new_wavelet, residual = call(
        k_final,
        (jax.ShapeDtypeStruct((2, f), F32), jax.ShapeDtypeStruct(modeled.shape, BF16)),
        [SM, SM] + [VM] * 5,
    )(me, line_of_slot, wd_here, wg_here, parts, wavelet, damping.reshape(1, f))
    return new_wavelet, residual


def solution(mesh):
    fine = Mesh(mesh.devices.reshape(2, 4, 2, 8, 2), ("xh", "y", "xl", "z", "c"))
    placed = (
        P(None, SHOT, None, RCV, None),
        P(None, SHOT, RCV, None, None),
        P(SHOT, None, RCV),
        P(),
        P(),
        P(),
        P(),
        P(),
    )
    return jax.shard_map(
        update,
        mesh=fine,
        in_specs=placed,
        out_specs=(P(), P(None, SHOT, None, RCV, None)),
        check_vma=False,
    )
```

```python
import jax
import jax.numpy as jnp
from jax import lax
from jax.experimental import pallas as pl
from jax.experimental.pallas import tpu as pltpu
from jax.sharding import Mesh, PartitionSpec as P

F32 = jnp.float32
BF16 = jnp.bfloat16
SHOT = ("xh", "yh", "yl")
RCV = ("xl", "zh", "zm", "zl", "c")
REST = ("xh", "yh", "xl", "zh")
SWAPS = (4, 5, 6, 7, 1, 2, 3)

VM = pl.BlockSpec(memory_space=pltpu.VMEM)
SM = pl.BlockSpec(memory_space=pltpu.SMEM)
ANY = pl.BlockSpec(memory_space=pl.ANY)
HBM = pl.BlockSpec(memory_space=pltpu.HBM)


def call(body, outs, in_specs, out_specs=None, scratch=(), limit=12 << 20, flops=0, nbytes=1 << 20):
    many = isinstance(outs, (tuple, list))
    return pl.pallas_call(
        body,
        out_shape=outs,
        in_specs=in_specs,
        out_specs=out_specs if out_specs is not None else ([VM] * len(outs) if many else VM),
        scratch_shapes=list(scratch),
        compiler_params=pltpu.CompilerParams(vmem_limit_bytes=limit),
        cost_estimate=pl.CostEstimate(flops=flops, bytes_accessed=nbytes, transcendentals=0),
    )


CHUNKS = 4
BIG = 62 << 20
MID = 40 << 20


def k_spread(obs_ref, out_ref, buf, sem_in, sem_out):
    parts, pieces = obs_ref.shape[:2]
    step = pieces // CHUNKS
    ins, outs = [], []
    for q in range(CHUNKS):
        rows = pl.ds(q * step, step)
        for i in range(parts):
            ins.append(pltpu.make_async_copy(obs_ref.at[i, rows], buf.at[rows, i], sem_in.at[q, i]))
        outs.append(pltpu.make_async_copy(buf.at[rows], out_ref.at[rows], sem_out.at[q]))
    for c in ins:
        c.start()
    for q in range(CHUNKS):
        for i in range(parts):
            ins[q * parts + i].wait()
        outs[q].start()
    for c in outs:
        c.wait()


def couple(c_ref, b_ref):
    f = c_ref.shape[1]
    re, im = c_ref[0], c_ref[1]
    b_ref[0, :f] = re
    b_ref[0, f:] = -im
    b_ref[1, :f] = im
    b_ref[1, f:] = re


def k_mask(me_ref, slot_ref, mod_ref, mask_ref, live_ref, *out_refs):
    me = me_ref[0]
    shots, rb = mod_ref.shape[1], mod_ref.shape[3]
    f = mod_ref.shape[4]
    eye = lax.broadcasted_iota(jnp.int32, (rb, rb), 0) == lax.broadcasted_iota(jnp.int32, (rb, rb), 1)
    for b, out_ref in enumerate(out_refs):
        line = slot_ref[lax.bitwise_xor(me, b)]
        for s in range(shots):
            row = mask_ref[s, pl.ds(line, 1)].astype(F32)
            column = jnp.where(eye, row, 0.0).sum(axis=1, keepdims=True)
            rows = pl.ds(s * rb, rb)
            live_ref[b, rows] = jnp.broadcast_to(column, (rb, 128))
            live = jnp.broadcast_to(column, (rb, f)) > 0.5
            for c in range(2):
                x = mod_ref[c, s, line].astype(F32)
                out_ref[c, rows] = jnp.where(live, x, 0.0).astype(BF16)


def window_out(x_ref, b_ref, out_ref, buf, sem):
    copies = []
    for d in range(2):
        w = jnp.dot(x_ref[...], b_ref[d], preferred_element_type=F32)
        buf[d] = w.reshape(buf.shape[1:])
        copies.append(pltpu.make_async_copy(buf.at[d], out_ref.at[d], sem.at[d]))
        if d:
            copies[d - 1].start()
    copies[-1].start()
    for c in copies:
        c.wait()


def k_window_here(*refs):
    xs, c_ref, out_ref, x_ref, b_ref, buf, sem = refs[:-6], *refs[-6:]
    couple(c_ref, b_ref)
    rows, f = xs[0].shape[1:]
    for b, x in enumerate(xs):
        for c in range(2):
            x_ref[b * rows : (b + 1) * rows, c * f : (c + 1) * f] = x[c]
    window_out(x_ref, b_ref, out_ref, buf, sem)


def k_window_own(me_ref, own_ref, live_ref, c_ref, out_ref, own, live, coup, x_ref, b_ref, buf, isem, sem):
    me = me_ref[0]
    ins = [
        pltpu.make_async_copy(src, dst, isem.at[i])
        for i, (src, dst) in enumerate(((c_ref, coup), (live_ref, live), (own_ref, own)))
    ]
    for c in ins:
        c.start()
    slots, _, rows, f = own_ref.shape
    ins[0].wait()
    couple(coup, b_ref)
    ins[1].wait()
    ins[2].wait()
    for b in range(slots):
        k = lax.bitwise_xor(me, b)
        alive = jnp.concatenate([live[b]] * (f // live.shape[2]), axis=1) > 0.5
        for c in range(2):
            x = own[k, c].astype(F32)
            x_ref[b * rows : (b + 1) * rows, c * f : (c + 1) * f] = jnp.where(alive, x, 0.0).astype(BF16)
    window_out(x_ref, b_ref, out_ref, buf, sem)


def k_group(order_ref, own_ref, out_ref, buf, isem, sem):
    groups, _, size = out_ref.shape[:3]
    for g in range(groups):
        for s in range(size):
            n = order_ref[g * size + s]
            j = lax.shift_right_logical(n, 1)
            h = lax.bitwise_and(n, 1)
            for c in range(2):
                pltpu.make_async_copy(own_ref.at[j, 2 * c + h], buf.at[g, c, s], isem.at[g]).start()
    copies = [pltpu.make_async_copy(buf.at[g], out_ref.at[g], sem.at[g]) for g in range(groups)]
    for g in range(groups):
        pltpu.make_async_copy(out_ref.at[g], buf.at[g], isem.at[g]).wait()
        copies[g].start()
    for c in copies:
        c.wait()


def fold(x):
    return x.reshape(x.shape[0] // 8, 8, x.shape[1]).sum(axis=0).sum(axis=0, keepdims=True)


def k_cross(me_ref, own_ref, c_ref, *refs):
    mods, (out_ref, x_ref, m_ref, coup, b_ref, csem, osem, msem) = refs[:-8], refs[-8:]
    me = me_ref[0]
    groups = len(mods)
    rows, f = mods[0].shape[1:]

    def rows_of(dst, b, c):
        return dst.at[pl.ds(b * rows, rows), pl.ds(c * f, f)]

    first = pltpu.make_async_copy(c_ref, coup, csem)
    first.start()
    pairs = [(b, c) for b in range(groups) for c in range(2)]
    owns = [
        pltpu.make_async_copy(own_ref.at[lax.bitwise_xor(me, b), c], rows_of(x_ref, b, c), osem.at[b, c])
        for b, c in pairs
    ]
    for c in owns:
        c.start()
    copies = [pltpu.make_async_copy(mods[b].at[c], rows_of(m_ref, b, c), msem.at[b, c]) for b, c in pairs]
    for c in copies:
        c.start()
    first.wait()
    couple(coup, b_ref)
    for c in owns:
        c.wait()
    wd_re = jnp.dot(x_ref[...], b_ref[0], preferred_element_type=F32)
    wd_im = jnp.dot(x_ref[...], b_ref[1], preferred_element_type=F32)
    for c in copies:
        c.wait()
    wg_re = jnp.dot(m_ref[...], b_ref[0], preferred_element_type=F32)
    wg_im = jnp.dot(m_ref[...], b_ref[1], preferred_element_type=F32)
    out_ref[0:1] = fold(wg_re * wd_re + wg_im * wd_im)
    out_ref[1:2] = fold(wg_re * wd_im - wg_im * wd_re)
    out_ref[2:3] = fold(wg_re * wg_re + wg_im * wg_im)


def k_final(me_ref, slot_ref, wd_ref, wg_ref, sums_ref, wav_ref, damp_ref, nw_ref, out_ref, wd, wg, buf, sem, osem):
    me = me_ref[0]
    _, lines, _, f = wd_ref.shape
    shots, rb = out_ref.shape[1], out_ref.shape[3]
    ins = [
        [
            pltpu.make_async_copy(src.at[:, b], dst.at[:, b], sem.at[i, b])
            for i, (src, dst) in enumerate(((wd_ref, wd), (wg_ref, wg)))
        ]
        for b in range(lines)
    ]
    for pair in ins:
        for c in pair:
            c.start()
    outs = [
        pltpu.make_async_copy(
            buf.at[b], out_ref.at[:, :, slot_ref[lax.bitwise_xor(me, b)]], osem.at[b]
        )
        for b in range(lines)
    ]
    total = sums_ref[...].sum(axis=0)
    cross_re, cross_im, den = total[:, :f], total[:, f : 2 * f], total[:, 2 * f :]
    wav_re, wav_im = wav_ref[0:1], wav_ref[1:2]
    scale = den + damp_ref[...]
    nw_re = wav_re + (cross_re - wav_re * den) / scale
    nw_im = wav_im + (cross_im - wav_im * den) / scale
    nw_ref[0:1] = nw_re
    nw_ref[1:2] = nw_im
    for b in range(lines):
        for c in ins[b]:
            c.wait()
        wg_re, wg_im = wg[0, b], wg[1, b]
        out_re = wd[0, b] - (nw_re * wg_re - nw_im * wg_im)
        out_im = wd[1, b] - (nw_re * wg_im + nw_im * wg_re)
        buf[b, 0] = out_re.reshape(shots, rb, f).astype(BF16)
        buf[b, 1] = out_im.reshape(shots, rb, f).astype(BF16)
        if b:
            outs[b - 1].start()
    outs[-1].start()
    for c in outs:
        c.wait()


def swapped(x, axis, bit):
    size = lax.axis_size(axis)
    return lax.ppermute(x, axis, [(i, i ^ bit) for i in range(size)])


def sent_to_all(array, axis):
    size = lax.axis_size(axis)
    return lax.all_to_all(
        jnp.broadcast_to(array[None], (size, *array.shape)), axis, 0, 0, tiled=True
    )


def update(modeled, observed, mask, shot_order, line_of_slot, coupling, wavelet, damping):
    _, shots, lines, rb, f = modeled.shape
    slots = lax.axis_size(SHOT)
    held = observed.shape[2]
    pieces = lax.axis_size(RCV)
    rows = shots * rb
    traces = lines * rows
    flops = 8 * traces * f * f
    me = lax.axis_index(SHOT).astype(jnp.int32).reshape(1)

    own_spread = call(
        k_spread, jax.ShapeDtypeStruct((pieces, 2 * held, rb, f), BF16), [ANY], HBM,
        limit=BIG,
        scratch=[
            pltpu.VMEM((pieces, 2 * held, rb, f), BF16),
            pltpu.SemaphoreType.DMA((CHUNKS, 2 * held)),
            pltpu.SemaphoreType.DMA((CHUNKS,)),
        ],
    )(observed.reshape(2 * held, pieces, rb, f))
    own_natural = lax.all_to_all(own_spread, RCV, 0, 0, tiled=True)

    piece = jax.ShapeDtypeStruct((2, rows, f), BF16)
    live, *masked = call(
        k_mask, (jax.ShapeDtypeStruct((slots, rows, 128), F32), *[piece] * slots),
        [SM, SM, VM, VM],
    )(me, line_of_slot, modeled, mask)
    wide = jax.ShapeDtypeStruct((2, slots, rows, f), F32)
    x_block = pltpu.VMEM((traces, 2 * f), BF16)
    b_block = pltpu.VMEM((2, 2 * f, f), BF16)
    window_scratch = [x_block, b_block, pltpu.VMEM((2, slots, rows, f), F32), pltpu.SemaphoreType.DMA((2,))]
    arrived = {0: masked[0]}
    for b in SWAPS:
        arrived[b] = swapped(masked[b], SHOT, b)
    wg_here = call(
        k_window_here, wide, [VM] * (slots + 1), HBM, flops=flops,
        scratch=window_scratch,
    )(*masked, coupling)

    own_group = call(
        k_group, jax.ShapeDtypeStruct((slots, 2, shots, rb, f), BF16), [SM, ANY], HBM,
        scratch=[
            pltpu.VMEM((slots, 2, shots, rb, f), BF16),
            pltpu.SemaphoreType.DMA((slots,)),
            pltpu.SemaphoreType.DMA((slots,)),
        ],
        limit=BIG,
    )(shot_order, own_natural).reshape(slots, 2, rows, f)
    own_here = lax.all_to_all(own_group, SHOT, 0, 0, tiled=True)
    coup = pltpu.VMEM(coupling.shape, BF16)
    sums = call(
        k_cross, jax.ShapeDtypeStruct((3, f), F32), [SM, ANY, ANY] + [ANY] * slots,
        scratch=[
            x_block, x_block, coup, b_block, pltpu.SemaphoreType.DMA,
            pltpu.SemaphoreType.DMA((slots, 2)), pltpu.SemaphoreType.DMA((slots, 2)),
        ],
        limit=MID, flops=2 * flops,
    )(me, own_group, coupling, *[arrived[b] for b in range(slots)])
    sums = sums.reshape(3 * f // 128, 128)
    for axis in ("c", "zl", "zm", "yl"):
        sums = sums + swapped(sums, axis, 1)
    parts = sent_to_all(sums.reshape(1, 3 * f), REST)
    wd_here = call(
        k_window_own, wide, [SM, ANY, ANY, ANY], HBM, flops=flops, limit=MID,
        scratch=[
            pltpu.VMEM(own_here.shape, BF16), pltpu.VMEM(live.shape, F32), coup, x_block, b_block,
            window_scratch[2], pltpu.SemaphoreType.DMA((3,)), pltpu.SemaphoreType.DMA((2,)),
        ],
    )(me, own_here, live, coupling)

    new_wavelet, residual = call(
        k_final,
        (jax.ShapeDtypeStruct((2, f), F32), jax.ShapeDtypeStruct(modeled.shape, BF16)),
        [SM, SM, ANY, ANY, VM, VM, VM], [VM, HBM],
        scratch=[
            pltpu.VMEM((2, slots, rows, f), F32),
            pltpu.VMEM((2, slots, rows, f), F32),
            pltpu.VMEM((slots, 2, shots, rb, f), BF16),
            pltpu.SemaphoreType.DMA((2, slots)),
            pltpu.SemaphoreType.DMA((slots,)),
        ],
        limit=MID,
    )(me, line_of_slot, wd_here, wg_here, parts, wavelet, damping.reshape(1, f))
    return new_wavelet, residual


def solution(mesh):
    fine = Mesh(mesh.devices.reshape((2,) * 8), SHOT + RCV)
    placed = (
        P(None, SHOT, None, RCV, None),
        P(None, SHOT, RCV, None, None),
        P(SHOT, None, RCV),
        P(),
        P(),
        P(),
        P(),
        P(),
    )
    return jax.shard_map(
        update,
        mesh=fine,
        in_specs=placed,
        out_specs=(P(), P(None, SHOT, None, RCV, None)),
        check_vma=False,
    )
```

```python
import jax
import jax.numpy as jnp
from jax import lax
from jax.experimental import pallas as pl
from jax.experimental.pallas import tpu as pltpu
from jax.sharding import Mesh, PartitionSpec as P

F32 = jnp.float32
BF16 = jnp.bfloat16
SHOT = ("xh", "yh", "yl")
RCV = ("xl", "zh", "zm", "zl", "c")
REST = ("xh", "yh", "yl", "xl")
SWAPS = (4, 5, 6, 7, 1, 2, 3)

VM = pl.BlockSpec(memory_space=pltpu.VMEM)
SM = pl.BlockSpec(memory_space=pltpu.SMEM)
ANY = pl.BlockSpec(memory_space=pl.ANY)
HBM = pl.BlockSpec(memory_space=pltpu.HBM)


def call(body, outs, in_specs, out_specs=None, scratch=(), limit=12 << 20, flops=0, nbytes=1 << 20):
    many = isinstance(outs, (tuple, list))
    return pl.pallas_call(
        body,
        out_shape=outs,
        in_specs=in_specs,
        out_specs=out_specs if out_specs is not None else ([VM] * len(outs) if many else VM),
        scratch_shapes=list(scratch),
        compiler_params=pltpu.CompilerParams(vmem_limit_bytes=limit),
        cost_estimate=pl.CostEstimate(flops=flops, bytes_accessed=nbytes, transcendentals=0),
    )


CHUNKS = 4
BIG = 62 << 20
MID = 40 << 20
WIN = 61 << 20
CRS = 50 << 20
FIN = 50 << 20


def k_spread(obs_ref, out_ref, buf, sem_in, sem_out):
    parts, pieces = obs_ref.shape[:2]
    held = parts // 2
    step = pieces // CHUNKS
    ins, outs = [], []
    for q in range(CHUNKS):
        rows = pl.ds(q * step, step)
        for i in range(parts):
            to = i % held * 2 + i // held
            ins.append(pltpu.make_async_copy(obs_ref.at[i, rows], buf.at[rows, to], sem_in.at[q, i]))
        outs.append(pltpu.make_async_copy(buf.at[rows], out_ref.at[rows], sem_out.at[q]))
    for c in ins:
        c.start()
    for q in range(CHUNKS):
        for i in range(parts):
            ins[q * parts + i].wait()
        outs[q].start()
    for c in outs:
        c.wait()


def couple(c_ref, b_ref):
    f = c_ref.shape[1]
    re, im = c_ref[0], c_ref[1]
    b_ref[0, :f] = re
    b_ref[0, f:] = -im
    b_ref[1, :f] = im
    b_ref[1, f:] = re


def k_mask(me_ref, slot_ref, mod_ref, mask_ref, live_ref, *out_refs):
    me = me_ref[0]
    shots, rb = mod_ref.shape[1], mod_ref.shape[3]
    f = mod_ref.shape[4]
    eye = lax.broadcasted_iota(jnp.int32, (rb, rb), 0) == lax.broadcasted_iota(jnp.int32, (rb, rb), 1)
    for b, out_ref in enumerate(out_refs):
        line = slot_ref[lax.bitwise_xor(me, b)]
        for s in range(shots):
            row = mask_ref[s, pl.ds(line, 1)].astype(F32)
            column = jnp.where(eye, row, 0.0).sum(axis=1, keepdims=True)
            rows = pl.ds(s * rb, rb)
            live_ref[b, rows] = jnp.broadcast_to(column, (rb, 128))
            live = jnp.broadcast_to(column, (rb, f)) > 0.5
            for c in range(2):
                x = mod_ref[c, s, line].astype(F32)
                out_ref[c, rows] = jnp.where(live, x, 0.0).astype(BF16)


def window(x_ref, b_ref, d):
    x = jnp.concatenate([x_ref[0], x_ref[1]], axis=1)
    return jnp.dot(x, b_ref[d], preferred_element_type=F32)


def window_out(x_ref, b_ref, out_ref, buf, sem):
    copies = []
    for d in range(2):
        buf[d] = window(x_ref, b_ref, d).reshape(buf.shape[1:])
        copies.append(pltpu.make_async_copy(buf.at[d], out_ref.at[d], sem.at[d]))
        if d:
            copies[d - 1].start()
    copies[-1].start()
    for c in copies:
        c.wait()


def k_window(*refs):
    xs, c_ref, (out_ref, coup, x_ref, b_ref, buf, csem, isem, sem) = refs[:-9], refs[-9], refs[-8:]
    rows = xs[0].shape[1]
    first = pltpu.make_async_copy(c_ref, coup, csem)
    first.start()
    ins = [
        pltpu.make_async_copy(x, x_ref.at[:, pl.ds(b * rows, rows)], isem.at[b])
        for b, x in enumerate(xs)
    ]
    for c in ins:
        c.start()
    first.wait()
    couple(coup, b_ref)
    for c in ins:
        c.wait()
    window_out(x_ref, b_ref, out_ref, buf, sem)


def k_window_own(me_ref, own_ref, live_ref, c_ref, out_ref, own, live, coup, x_ref, b_ref, buf, isem, sem):
    me = me_ref[0]
    ins = [
        pltpu.make_async_copy(src, dst, isem.at[i])
        for i, (src, dst) in enumerate(((c_ref, coup), (live_ref, live), (own_ref, own)))
    ]
    for c in ins:
        c.start()
    slots, _, rows, f = own_ref.shape
    ins[0].wait()
    couple(coup, b_ref)
    ins[1].wait()
    ins[2].wait()
    for b in range(slots):
        k = lax.bitwise_xor(me, b)
        alive = jnp.concatenate([live[b]] * (f // live.shape[2]), axis=1) > 0.5
        for c in range(2):
            x = own[k, c].astype(F32)
            x_ref[c, b * rows : (b + 1) * rows] = jnp.where(alive, x, 0.0).astype(BF16)
    window_out(x_ref, b_ref, out_ref, buf, sem)


def fold(x):
    return x.reshape(x.shape[0] // 8, 8, x.shape[1]).sum(axis=0).sum(axis=0, keepdims=True)


def k_cross(me_ref, order_ref, own_ref, c_ref, wg_ref, sum_ref, out_ref, coup, wg, x_ref, b_ref, csem, wsem, isem, osem):
    me = me_ref[0]
    rb, _ = own_ref.shape[3:]
    groups, _, rows, _ = out_ref.shape
    size = rows // rb
    first = pltpu.make_async_copy(c_ref, coup, csem)
    first.start()
    for b in range(groups):
        g = lax.bitwise_xor(me, b)
        for s in range(size):
            n = order_ref[g * size + s]
            j = lax.shift_right_logical(n, 1)
            h = lax.bitwise_and(n, 1)
            to = pl.ds((b * size + s) * rb, rb)
            pltpu.make_async_copy(own_ref.at[j, h], x_ref.at[:, to], isem.at[b]).start()
    wgs = [pltpu.make_async_copy(wg_ref.at[d], wg.at[d], wsem.at[d]) for d in range(2)]
    for c in wgs:
        c.start()
    first.wait()
    couple(coup, b_ref)
    outs = []
    for b in range(groups):
        part = x_ref.at[:, pl.ds(b * rows, rows)]
        pltpu.make_async_copy(part, part, isem.at[b]).wait()
        outs.append(pltpu.make_async_copy(part, out_ref.at[lax.bitwise_xor(me, b)], osem.at[b]))
        outs[b].start()
    wd_re = window(x_ref, b_ref, 0)
    wd_im = window(x_ref, b_ref, 1)
    for c in wgs:
        c.wait()
    wg_re, wg_im = wg[0].reshape(wd_re.shape), wg[1].reshape(wd_re.shape)
    sum_ref[0:1] = fold(wg_re * wd_re + wg_im * wd_im)
    sum_ref[1:2] = fold(wg_re * wd_im - wg_im * wd_re)
    sum_ref[2:3] = fold(wg_re * wg_re + wg_im * wg_im)
    for c in outs:
        c.wait()


def k_final(me_ref, slot_ref, wd_ref, wg_ref, sums_ref, wav_ref, damp_ref, nw_ref, out_ref, wd, wg, buf, sem, osem):
    me = me_ref[0]
    _, lines, _, f = wd_ref.shape
    shots, rb = out_ref.shape[1], out_ref.shape[3]
    ins = [
        [
            pltpu.make_async_copy(src.at[:, b], dst.at[:, b], sem.at[i, b])
            for i, (src, dst) in enumerate(((wd_ref, wd), (wg_ref, wg)))
        ]
        for b in range(lines)
    ]
    for pair in ins:
        for c in pair:
            c.start()
    outs = [
        pltpu.make_async_copy(
            buf.at[b], out_ref.at[:, :, slot_ref[lax.bitwise_xor(me, b)]], osem.at[b]
        )
        for b in range(lines)
    ]
    total = sums_ref[...].sum(axis=0)
    cross_re, cross_im, den = total[:, :f], total[:, f : 2 * f], total[:, 2 * f :]
    wav_re, wav_im = wav_ref[0:1], wav_ref[1:2]
    scale = den + damp_ref[...]
    nw_re = wav_re + (cross_re - wav_re * den) / scale
    nw_im = wav_im + (cross_im - wav_im * den) / scale
    nw_ref[0:1] = nw_re
    nw_ref[1:2] = nw_im
    for b in range(lines):
        for c in ins[b]:
            c.wait()
        wg_re, wg_im = wg[0, b], wg[1, b]
        out_re = wd[0, b] - (nw_re * wg_re - nw_im * wg_im)
        out_im = wd[1, b] - (nw_re * wg_im + nw_im * wg_re)
        buf[b, 0] = out_re.reshape(shots, rb, f).astype(BF16)
        buf[b, 1] = out_im.reshape(shots, rb, f).astype(BF16)
        if b:
            outs[b - 1].start()
    outs[-1].start()
    for c in outs:
        c.wait()


def swapped(x, axis, bit):
    size = lax.axis_size(axis)
    return lax.ppermute(x, axis, [(i, i ^ bit) for i in range(size)])


def sent_to_all(array, axis):
    size = lax.axis_size(axis)
    return lax.all_to_all(
        jnp.broadcast_to(array[None], (size, *array.shape)), axis, 0, 0, tiled=True
    )


def update(modeled, observed, mask, shot_order, line_of_slot, coupling, wavelet, damping):
    _, shots, lines, rb, f = modeled.shape
    slots = lax.axis_size(SHOT)
    held = observed.shape[2]
    pieces = lax.axis_size(RCV)
    rows = shots * rb
    traces = lines * rows
    flops = 8 * traces * f * f
    me = lax.axis_index(SHOT).astype(jnp.int32).reshape(1)

    own_spread = call(
        k_spread, jax.ShapeDtypeStruct((pieces, 2 * held, rb, f), BF16), [ANY], HBM,
        limit=BIG,
        scratch=[
            pltpu.VMEM((pieces, 2 * held, rb, f), BF16),
            pltpu.SemaphoreType.DMA((CHUNKS, 2 * held)),
            pltpu.SemaphoreType.DMA((CHUNKS,)),
        ],
    )(observed.reshape(2 * held, pieces, rb, f))
    own_natural = lax.all_to_all(own_spread, RCV, 0, 0, tiled=True)

    piece = jax.ShapeDtypeStruct((2, rows, f), BF16)
    live, *masked = call(
        k_mask, (jax.ShapeDtypeStruct((slots, rows, 128), F32), *[piece] * slots),
        [SM, SM, VM, VM],
    )(me, line_of_slot, modeled, mask)
    wide = jax.ShapeDtypeStruct((2, slots, rows, f), F32)
    dma = pltpu.SemaphoreType.DMA
    coup = pltpu.VMEM(coupling.shape, BF16)
    x_block = pltpu.VMEM((2, traces, f), BF16)
    b_block = pltpu.VMEM((2, 2 * f, f), BF16)
    w_block = pltpu.VMEM(wide.shape, F32)
    window_scratch = [coup, x_block, b_block, w_block, dma, dma((slots,)), dma((2,))]
    arrived = {0: masked[0]}
    for b in SWAPS:
        arrived[b] = swapped(masked[b], SHOT, b)
    wg_here = call(
        k_window, wide, [ANY] * (slots + 1), HBM, flops=flops,
        scratch=window_scratch, limit=WIN,
    )(*masked, coupling)
    wg_slot = call(
        k_window, wide, [ANY] * (slots + 1), HBM, flops=flops,
        scratch=window_scratch, limit=WIN,
    )(*[arrived[b] for b in range(slots)], coupling)

    sums, own_group = call(
        k_cross,
        (jax.ShapeDtypeStruct((3, f), F32), jax.ShapeDtypeStruct((slots, 2, rows, f), BF16)),
        [SM, SM, ANY, ANY, HBM], [VM, HBM],
        scratch=[coup, w_block, x_block, b_block, dma, dma((2,)), dma((slots,)), dma((slots,))],
        limit=CRS, flops=flops,
    )(me, shot_order, own_natural.reshape(pieces, held, 2, rb, f), coupling, wg_slot)
    own_here = lax.all_to_all(own_group, SHOT, 0, 0, tiled=True)
    sums = sums.reshape(3 * f // 128, 128)
    for axis in ("c", "zl", "zm", "zh"):
        sums = sums + swapped(sums, axis, 1)
    parts = sent_to_all(sums.reshape(1, 3 * f), REST)
    wd_here = call(
        k_window_own, wide, [SM, ANY, ANY, ANY], HBM, flops=flops, limit=MID,
        scratch=[
            pltpu.VMEM(own_here.shape, BF16), pltpu.VMEM(live.shape, F32), coup, x_block, b_block,
            w_block, dma((3,)), dma((2,)),
        ],
    )(me, own_here, live, coupling)

    new_wavelet, residual = call(
        k_final,
        (jax.ShapeDtypeStruct((2, f), F32), jax.ShapeDtypeStruct(modeled.shape, BF16)),
        [SM, SM, HBM, HBM, VM, VM, VM], [VM, HBM],
        scratch=[
            pltpu.VMEM((2, slots, rows, f), F32),
            pltpu.VMEM((2, slots, rows, f), F32),
            pltpu.VMEM((slots, 2, shots, rb, f), BF16),
            pltpu.SemaphoreType.DMA((2, slots)),
            pltpu.SemaphoreType.DMA((slots,)),
        ],
        limit=FIN,
    )(me, line_of_slot, wd_here, wg_here, parts, wavelet, damping.reshape(1, f))
    return new_wavelet, residual


def solution(mesh):
    fine = Mesh(mesh.devices.reshape((2,) * 8), SHOT + RCV)
    placed = (
        P(None, SHOT, None, RCV, None),
        P(None, SHOT, RCV, None, None),
        P(SHOT, None, RCV),
        P(),
        P(),
        P(),
        P(),
        P(),
    )
    return jax.shard_map(
        update,
        mesh=fine,
        in_specs=placed,
        out_specs=(P(), P(None, SHOT, None, RCV, None)),
        check_vma=False,
    )
```

```python
import jax
import jax.numpy as jnp
from jax import lax
from jax.experimental import pallas as pl
from jax.experimental.pallas import tpu as pltpu
from jax.sharding import Mesh, PartitionSpec as P

F32 = jnp.float32
BF16 = jnp.bfloat16
SHOT = ("xh", "yh", "yl")
RCV = ("xl", "zh", "zm", "zl", "c")
REST = ("xh", "yh", "yl", "xl")
SWAPS = (4, 5, 6, 7, 1, 2, 3)

VM = pl.BlockSpec(memory_space=pltpu.VMEM)
SM = pl.BlockSpec(memory_space=pltpu.SMEM)
ANY = pl.BlockSpec(memory_space=pl.ANY)
HBM = pl.BlockSpec(memory_space=pltpu.HBM)


def call(body, outs, in_specs, out_specs=None, scratch=(), limit=12 << 20, flops=0, nbytes=1 << 20):
    many = isinstance(outs, (tuple, list))
    return pl.pallas_call(
        body,
        out_shape=outs,
        in_specs=in_specs,
        out_specs=out_specs if out_specs is not None else ([VM] * len(outs) if many else VM),
        scratch_shapes=list(scratch),
        compiler_params=pltpu.CompilerParams(vmem_limit_bytes=limit),
        cost_estimate=pl.CostEstimate(flops=flops, bytes_accessed=nbytes, transcendentals=0),
    )


CHUNKS = 4
BIG = 62 << 20
MID = 40 << 20
WIN = 61 << 20
CRS = 50 << 20
GRP = 51 << 20
FIN = 50 << 20


def k_spread(obs_ref, out_ref, buf, sem_in, sem_out):
    parts, pieces = obs_ref.shape[:2]
    held = parts // 2
    step = pieces // CHUNKS
    ins, outs = [], []
    for q in range(CHUNKS):
        rows = pl.ds(q * step, step)
        for i in range(parts):
            to = i % held * 2 + i // held
            ins.append(pltpu.make_async_copy(obs_ref.at[i, rows], buf.at[rows, to], sem_in.at[q, i]))
        outs.append(pltpu.make_async_copy(buf.at[rows], out_ref.at[rows], sem_out.at[q]))
    for c in ins:
        c.start()
    for q in range(CHUNKS):
        for i in range(parts):
            ins[q * parts + i].wait()
        outs[q].start()
    for c in outs:
        c.wait()


def couple(c_ref, b_ref):
    f = c_ref.shape[1]
    re, im = c_ref[0], c_ref[1]
    b_ref[0, :f] = re
    b_ref[0, f:] = -im
    b_ref[1, :f] = im
    b_ref[1, f:] = re


def k_mask(me_ref, slot_ref, mod_ref, mask_ref, live_ref, *out_refs):
    me = me_ref[0]
    shots, rb = mod_ref.shape[1], mod_ref.shape[3]
    f = mod_ref.shape[4]
    eye = lax.broadcasted_iota(jnp.int32, (rb, rb), 0) == lax.broadcasted_iota(jnp.int32, (rb, rb), 1)
    for b, out_ref in enumerate(out_refs):
        line = slot_ref[lax.bitwise_xor(me, b)]
        for s in range(shots):
            row = mask_ref[s, pl.ds(line, 1)].astype(F32)
            column = jnp.where(eye, row, 0.0).sum(axis=1, keepdims=True)
            rows = pl.ds(s * rb, rb)
            live_ref[b, rows] = jnp.broadcast_to(column, (rb, 128))
            live = jnp.broadcast_to(column, (rb, f)) > 0.5
            for c in range(2):
                x = mod_ref[c, s, line].astype(F32)
                out_ref[c, rows] = jnp.where(live, x, 0.0).astype(BF16)


def window(x_ref, b_ref, d):
    x = jnp.concatenate([x_ref[0], x_ref[1]], axis=1)
    return jnp.dot(x, b_ref[d], preferred_element_type=F32)


def window_out(x_ref, b_ref, out_ref, buf, sem):
    copies = []
    for d in range(2):
        buf[d] = window(x_ref, b_ref, d).reshape(buf.shape[1:])
        copies.append(pltpu.make_async_copy(buf.at[d], out_ref.at[d], sem.at[d]))
        if d:
            copies[d - 1].start()
    copies[-1].start()
    for c in copies:
        c.wait()


def k_window(*refs):
    xs, c_ref, (out_ref, coup, x_ref, b_ref, buf, csem, isem, sem) = refs[:-9], refs[-9], refs[-8:]
    rows = xs[0].shape[1]
    first = pltpu.make_async_copy(c_ref, coup, csem)
    first.start()
    ins = [
        pltpu.make_async_copy(x, x_ref.at[:, pl.ds(b * rows, rows)], isem.at[b])
        for b, x in enumerate(xs)
    ]
    for c in ins:
        c.start()
    first.wait()
    couple(coup, b_ref)
    for c in ins:
        c.wait()
    window_out(x_ref, b_ref, out_ref, buf, sem)


def k_window_own(me_ref, own_ref, live_ref, c_ref, out_ref, own, live, coup, x_ref, b_ref, buf, isem, sem):
    me = me_ref[0]
    ins = [
        pltpu.make_async_copy(src, dst, isem.at[i])
        for i, (src, dst) in enumerate(((c_ref, coup), (live_ref, live), (own_ref, own)))
    ]
    for c in ins:
        c.start()
    slots, _, rows, f = own_ref.shape
    ins[0].wait()
    couple(coup, b_ref)
    ins[1].wait()
    ins[2].wait()
    for b in range(slots):
        k = lax.bitwise_xor(me, b)
        alive = jnp.concatenate([live[b]] * (f // live.shape[2]), axis=1) > 0.5
        for c in range(2):
            x = own[k, c].astype(F32)
            x_ref[c, b * rows : (b + 1) * rows] = jnp.where(alive, x, 0.0).astype(BF16)
    window_out(x_ref, b_ref, out_ref, buf, sem)


def fold(x):
    return x.reshape(x.shape[0] // 8, 8, x.shape[1]).sum(axis=0).sum(axis=0, keepdims=True)


def k_group(order_ref, own_ref, out_ref, buf, sem):
    groups, _, rows, _ = out_ref.shape
    rb = own_ref.shape[3]
    size = rows // rb
    copies = [pltpu.make_async_copy(buf.at[g], out_ref.at[g], sem.at[g]) for g in range(groups)]
    for g in range(groups):
        for s in range(size):
            n = order_ref[g * size + s]
            j = lax.shift_right_logical(n, 1)
            h = lax.bitwise_and(n, 1)
            for c in range(2):
                buf[g, c, s * rb : (s + 1) * rb] = own_ref[j, h, c]
        if g:
            copies[g - 1].start()
    copies[-1].start()
    for c in copies:
        c.wait()


def k_cross(me_ref, own_ref, c_ref, *refs):
    mods, (sum_ref, coup, x_ref, m_ref, b_ref, csem, osem, msem) = refs[:-8], refs[-8:]
    me = me_ref[0]
    groups = len(mods)
    rows = mods[0].shape[1]
    first = pltpu.make_async_copy(c_ref, coup, csem)
    first.start()
    owns = [
        pltpu.make_async_copy(
            own_ref.at[lax.bitwise_xor(me, b)], x_ref.at[:, pl.ds(b * rows, rows)], osem.at[b]
        )
        for b in range(groups)
    ]
    for c in owns:
        c.start()
    copies = [
        pltpu.make_async_copy(mods[b], m_ref.at[:, pl.ds(b * rows, rows)], msem.at[b])
        for b in range(groups)
    ]
    for c in copies:
        c.start()
    first.wait()
    couple(coup, b_ref)
    for c in owns:
        c.wait()
    wd_re = window(x_ref, b_ref, 0)
    wd_im = window(x_ref, b_ref, 1)
    for c in copies:
        c.wait()
    wg_re = window(m_ref, b_ref, 0)
    wg_im = window(m_ref, b_ref, 1)
    sum_ref[0:1] = fold(wg_re * wd_re + wg_im * wd_im)
    sum_ref[1:2] = fold(wg_re * wd_im - wg_im * wd_re)
    sum_ref[2:3] = fold(wg_re * wg_re + wg_im * wg_im)


def k_final(me_ref, slot_ref, wd_ref, wg_ref, sums_ref, wav_ref, damp_ref, nw_ref, out_ref, wd, wg, buf, sem, osem):
    me = me_ref[0]
    _, lines, _, f = wd_ref.shape
    shots, rb = out_ref.shape[1], out_ref.shape[3]
    ins = [
        [
            pltpu.make_async_copy(src.at[:, b], dst.at[:, b], sem.at[i, b])
            for i, (src, dst) in enumerate(((wd_ref, wd), (wg_ref, wg)))
        ]
        for b in range(lines)
    ]
    for pair in ins:
        for c in pair:
            c.start()
    outs = [
        pltpu.make_async_copy(
            buf.at[b], out_ref.at[:, :, slot_ref[lax.bitwise_xor(me, b)]], osem.at[b]
        )
        for b in range(lines)
    ]
    total = sums_ref[...].sum(axis=0)
    cross_re, cross_im, den = total[:, :f], total[:, f : 2 * f], total[:, 2 * f :]
    wav_re, wav_im = wav_ref[0:1], wav_ref[1:2]
    scale = den + damp_ref[...]
    nw_re = wav_re + (cross_re - wav_re * den) / scale
    nw_im = wav_im + (cross_im - wav_im * den) / scale
    nw_ref[0:1] = nw_re
    nw_ref[1:2] = nw_im
    for b in range(lines):
        for c in ins[b]:
            c.wait()
        wg_re, wg_im = wg[0, b], wg[1, b]
        out_re = wd[0, b] - (nw_re * wg_re - nw_im * wg_im)
        out_im = wd[1, b] - (nw_re * wg_im + nw_im * wg_re)
        buf[b, 0] = out_re.reshape(shots, rb, f).astype(BF16)
        buf[b, 1] = out_im.reshape(shots, rb, f).astype(BF16)
        if b:
            outs[b - 1].start()
    outs[-1].start()
    for c in outs:
        c.wait()


def swapped(x, axis, bit):
    size = lax.axis_size(axis)
    return lax.ppermute(x, axis, [(i, i ^ bit) for i in range(size)])


def sent_to_all(array, axis):
    size = lax.axis_size(axis)
    return lax.all_to_all(
        jnp.broadcast_to(array[None], (size, *array.shape)), axis, 0, 0, tiled=True
    )


def update(modeled, observed, mask, shot_order, line_of_slot, coupling, wavelet, damping):
    _, shots, lines, rb, f = modeled.shape
    slots = lax.axis_size(SHOT)
    held = observed.shape[2]
    pieces = lax.axis_size(RCV)
    rows = shots * rb
    traces = lines * rows
    flops = 8 * traces * f * f
    me = lax.axis_index(SHOT).astype(jnp.int32).reshape(1)

    own_spread = call(
        k_spread, jax.ShapeDtypeStruct((pieces, 2 * held, rb, f), BF16), [ANY], HBM,
        limit=BIG,
        scratch=[
            pltpu.VMEM((pieces, 2 * held, rb, f), BF16),
            pltpu.SemaphoreType.DMA((CHUNKS, 2 * held)),
            pltpu.SemaphoreType.DMA((CHUNKS,)),
        ],
    )(observed.reshape(2 * held, pieces, rb, f))
    own_natural = lax.all_to_all(own_spread, RCV, 0, 0, tiled=True)

    piece = jax.ShapeDtypeStruct((2, rows, f), BF16)
    live, *masked = call(
        k_mask, (jax.ShapeDtypeStruct((slots, rows, 128), F32), *[piece] * slots),
        [SM, SM, VM, VM],
    )(me, line_of_slot, modeled, mask)
    wide = jax.ShapeDtypeStruct((2, slots, rows, f), F32)
    dma = pltpu.SemaphoreType.DMA
    coup = pltpu.VMEM(coupling.shape, BF16)
    x_block = pltpu.VMEM((2, traces, f), BF16)
    b_block = pltpu.VMEM((2, 2 * f, f), BF16)
    w_block = pltpu.VMEM(wide.shape, F32)
    window_scratch = [coup, x_block, b_block, w_block, dma, dma((slots,)), dma((2,))]
    arrived = {0: masked[0]}
    for b in SWAPS:
        arrived[b] = swapped(masked[b], SHOT, b)
    wg_here = call(
        k_window, wide, [ANY] * (slots + 1), HBM, flops=flops,
        scratch=window_scratch, limit=WIN,
    )(*masked, coupling)
    own_group = call(
        k_group, jax.ShapeDtypeStruct((slots, 2, rows, f), BF16), [SM, VM], HBM,
        scratch=[pltpu.VMEM((slots, 2, rows, f), BF16), dma((slots,))], limit=GRP,
    )(shot_order, own_natural.reshape(pieces, held, 2, rb, f))
    own_here = lax.all_to_all(own_group, SHOT, 0, 0, tiled=True)
    sums = call(
        k_cross, jax.ShapeDtypeStruct((3, f), F32), [SM] + [ANY] * (slots + 2),
        scratch=[coup, x_block, x_block, b_block, dma, dma((slots,)), dma((slots,))],
        limit=CRS, flops=2 * flops,
    )(me, own_group, coupling, *[arrived[b] for b in range(slots)])
    sums = sums.reshape(3 * f // 128, 128)
    for axis in ("c", "zl"):
        sums = sums + swapped(sums, axis, 1)
    others = {}
    for bit in (2, 1, 3):
        others[bit] = swapped(sums, ("zh", "zm"), bit)
    sums = (sums + others[1]) + (others[2] + others[3])
    parts = sent_to_all(sums.reshape(1, 3 * f), REST)
    wd_here = call(
        k_window_own, wide, [SM, ANY, ANY, ANY], HBM, flops=flops, limit=MID,
        scratch=[
            pltpu.VMEM(own_here.shape, BF16), pltpu.VMEM(live.shape, F32), coup, x_block, b_block,
            w_block, dma((3,)), dma((2,)),
        ],
    )(me, own_here, live, coupling)

    new_wavelet, residual = call(
        k_final,
        (jax.ShapeDtypeStruct((2, f), F32), jax.ShapeDtypeStruct(modeled.shape, BF16)),
        [SM, SM, HBM, HBM, VM, VM, VM], [VM, HBM],
        scratch=[
            pltpu.VMEM((2, slots, rows, f), F32),
            pltpu.VMEM((2, slots, rows, f), F32),
            pltpu.VMEM((slots, 2, shots, rb, f), BF16),
            pltpu.SemaphoreType.DMA((2, slots)),
            pltpu.SemaphoreType.DMA((slots,)),
        ],
        limit=FIN,
    )(me, line_of_slot, wd_here, wg_here, parts, wavelet, damping.reshape(1, f))
    return new_wavelet, residual


def solution(mesh):
    fine = Mesh(mesh.devices.reshape((2,) * 8), SHOT + RCV)
    placed = (
        P(None, SHOT, None, RCV, None),
        P(None, SHOT, RCV, None, None),
        P(SHOT, None, RCV),
        P(),
        P(),
        P(),
        P(),
        P(),
    )
    return jax.shard_map(
        update,
        mesh=fine,
        in_specs=placed,
        out_specs=(P(), P(None, SHOT, None, RCV, None)),
        check_vma=False,
    )
```

```python
import jax
import jax.numpy as jnp
from jax import lax
from jax.experimental import pallas as pl
from jax.experimental.pallas import tpu as pltpu
from jax.sharding import Mesh, PartitionSpec as P

F32 = jnp.float32
BF16 = jnp.bfloat16
SHOT = ("xh", "yh", "yl")
RCV = ("xl", "zh", "zm", "zl", "c")
REST = ("xh", "yh", "yl", "xl")
SWAPS = (4, 5, 6, 7, 1, 2, 3)

VM = pl.BlockSpec(memory_space=pltpu.VMEM)
SM = pl.BlockSpec(memory_space=pltpu.SMEM)
ANY = pl.BlockSpec(memory_space=pl.ANY)
HBM = pl.BlockSpec(memory_space=pltpu.HBM)


def call(body, outs, in_specs, out_specs=None, scratch=(), limit=12 << 20, flops=0, nbytes=1 << 20):
    many = isinstance(outs, (tuple, list))
    return pl.pallas_call(
        body,
        out_shape=outs,
        in_specs=in_specs,
        out_specs=out_specs if out_specs is not None else ([VM] * len(outs) if many else VM),
        scratch_shapes=list(scratch),
        compiler_params=pltpu.CompilerParams(vmem_limit_bytes=limit),
        cost_estimate=pl.CostEstimate(flops=flops, bytes_accessed=nbytes, transcendentals=0),
    )


CHUNKS = 4
BIG = 62 << 20
MID = 40 << 20
WIN = 61 << 20
CRS = 50 << 20
GRP = 51 << 20
FIN = 50 << 20


def k_spread(obs_ref, out_ref, buf, sem_in, sem_out):
    parts, pieces = obs_ref.shape[:2]
    held = parts // 2
    step = pieces // CHUNKS
    ins, outs = [], []
    for q in range(CHUNKS):
        rows = pl.ds(q * step, step)
        for i in range(parts):
            to = i % held * 2 + i // held
            ins.append(pltpu.make_async_copy(obs_ref.at[i, rows], buf.at[rows, to], sem_in.at[q, i]))
        outs.append(pltpu.make_async_copy(buf.at[rows], out_ref.at[rows], sem_out.at[q]))
    for c in ins:
        c.start()
    for q in range(CHUNKS):
        for i in range(parts):
            ins[q * parts + i].wait()
        outs[q].start()
    for c in outs:
        c.wait()


def couple(c_ref, b_ref):
    f = c_ref.shape[1]
    re, im = c_ref[0], c_ref[1]
    b_ref[0, :f] = re
    b_ref[0, f:] = -im
    b_ref[1, :f] = im
    b_ref[1, f:] = re


def k_mask(me_ref, slot_ref, mod_ref, mask_ref, live_ref, *out_refs):
    me = me_ref[0]
    shots, rb = mod_ref.shape[1], mod_ref.shape[3]
    f = mod_ref.shape[4]
    eye = lax.broadcasted_iota(jnp.int32, (rb, rb), 0) == lax.broadcasted_iota(jnp.int32, (rb, rb), 1)
    for b, out_ref in enumerate(out_refs):
        line = slot_ref[lax.bitwise_xor(me, b)]
        for s in range(shots):
            row = mask_ref[s, pl.ds(line, 1)].astype(F32)
            column = jnp.where(eye, row, 0.0).sum(axis=1, keepdims=True)
            rows = pl.ds(s * rb, rb)
            live_ref[b, rows] = jnp.broadcast_to(column, (rb, 128))
            live = jnp.broadcast_to(column, (rb, f)) > 0.5
            for c in range(2):
                x = mod_ref[c, s, line].astype(F32)
                out_ref[c, rows] = jnp.where(live, x, 0.0).astype(BF16)


def window(x_ref, b_ref, d):
    x = jnp.concatenate([x_ref[0], x_ref[1]], axis=1)
    return jnp.dot(x, b_ref[d], preferred_element_type=F32)


def window_out(x_ref, b_ref, out_ref, buf, sem):
    copies = []
    for d in range(2):
        buf[d] = window(x_ref, b_ref, d).reshape(buf.shape[1:])
        copies.append(pltpu.make_async_copy(buf.at[d], out_ref.at[d], sem.at[d]))
        if d:
            copies[d - 1].start()
    copies[-1].start()
    for c in copies:
        c.wait()


def k_window(*refs):
    xs, c_ref, (out_ref, coup, x_ref, b_ref, buf, csem, isem, sem) = refs[:-9], refs[-9], refs[-8:]
    rows = xs[0].shape[1]
    first = pltpu.make_async_copy(c_ref, coup, csem)
    first.start()
    ins = [
        pltpu.make_async_copy(x, x_ref.at[:, pl.ds(b * rows, rows)], isem.at[b])
        for b, x in enumerate(xs)
    ]
    for c in ins:
        c.start()
    first.wait()
    couple(coup, b_ref)
    for c in ins:
        c.wait()
    window_out(x_ref, b_ref, out_ref, buf, sem)


def k_window_own(me_ref, own_ref, live_ref, c_ref, out_ref, own, live, coup, x_ref, b_ref, buf, isem, sem):
    me = me_ref[0]
    ins = [
        pltpu.make_async_copy(src, dst, isem.at[i])
        for i, (src, dst) in enumerate(((c_ref, coup), (live_ref, live), (own_ref, own)))
    ]
    for c in ins:
        c.start()
    slots, _, rows, f = own_ref.shape
    ins[0].wait()
    couple(coup, b_ref)
    ins[1].wait()
    ins[2].wait()
    for b in range(slots):
        k = lax.bitwise_xor(me, b)
        alive = jnp.concatenate([live[b]] * (f // live.shape[2]), axis=1) > 0.5
        for c in range(2):
            x = own[k, c].astype(F32)
            x_ref[c, b * rows : (b + 1) * rows] = jnp.where(alive, x, 0.0).astype(BF16)
    window_out(x_ref, b_ref, out_ref, buf, sem)


def fold(x):
    return x.reshape(x.shape[0] // 8, 8, x.shape[1]).sum(axis=0).sum(axis=0, keepdims=True)


def k_group(order_ref, own_ref, out_ref, buf, sem):
    groups, _, rows, _ = out_ref.shape
    rb = own_ref.shape[3]
    size = rows // rb
    copies = [pltpu.make_async_copy(buf.at[g], out_ref.at[g], sem.at[g]) for g in range(groups)]
    for g in range(groups):
        for s in range(size):
            n = order_ref[g * size + s]
            j = lax.shift_right_logical(n, 1)
            h = lax.bitwise_and(n, 1)
            for c in range(2):
                buf[g, c, s * rb : (s + 1) * rb] = own_ref[j, h, c]
        if g:
            copies[g - 1].start()
    copies[-1].start()
    for c in copies:
        c.wait()


def k_cross(me_ref, order_ref, own_ref, c_ref, *refs):
    mods, (sum_ref, x_ref, m_ref, b_ref, sem) = refs[:-5], refs[-5:]
    me = me_ref[0]
    groups = len(mods)
    rows, f = mods[0].shape[1:]
    rb = own_ref.shape[3]
    size = rows // rb
    copies = [
        pltpu.make_async_copy(mods[b], m_ref.at[:, pl.ds(b * rows, rows)], sem.at[b])
        for b in range(groups)
    ]
    for c in copies:
        c.start()
    def couple_rows(i, carry):
        block = f // 4
        upper, lower = pl.ds(pl.multiple_of(i * block, block), block), pl.ds(pl.multiple_of(f + i * block, block), block)
        re, im = c_ref[0, upper], c_ref[1, upper]
        b_ref[0, upper] = re
        b_ref[0, lower] = -im
        b_ref[1, upper] = im
        b_ref[1, lower] = re
        return carry

    lax.fori_loop(0, 4, couple_rows, 0)
    for b in range(groups):
        g = lax.bitwise_xor(me, b)
        for s in range(size):
            n = order_ref[g * size + s]
            j = lax.shift_right_logical(n, 1)
            h = lax.bitwise_and(n, 1)
            row = (b * size + s) * rb
            for c in range(2):
                x_ref[c, row : row + rb] = own_ref[j, h, c]
    wd_re, wd_im = window(x_ref, b_ref, 0), window(x_ref, b_ref, 1)
    for c in copies:
        c.wait()
    wg_re, wg_im = window(m_ref, b_ref, 0), window(m_ref, b_ref, 1)
    sum_ref[0:1] = fold(wg_re * wd_re + wg_im * wd_im)
    sum_ref[1:2] = fold(wg_re * wd_im - wg_im * wd_re)
    sum_ref[2:3] = fold(wg_re * wg_re + wg_im * wg_im)


def k_final(me_ref, slot_ref, wd, wg_ref, sums_ref, wav_ref, damp_ref, nw_ref, out_ref, wg, buf, nw, sem, osem, nsem):
    me = me_ref[0]
    _, lines, _, f = wg_ref.shape
    shots, rb = out_ref.shape[1], out_ref.shape[3]
    ins = [pltpu.make_async_copy(wg_ref.at[:, b], wg.at[:, b], sem.at[b]) for b in range(lines)]
    for c in ins:
        c.start()
    outs = [
        pltpu.make_async_copy(
            buf.at[b], out_ref.at[:, :, slot_ref[lax.bitwise_xor(me, b)]], osem.at[b]
        )
        for b in range(lines)
    ]
    total = sums_ref[...].sum(axis=0)
    cross_re, cross_im, den = total[:, :f], total[:, f : 2 * f], total[:, 2 * f :]
    wav_re, wav_im = wav_ref[0:1], wav_ref[1:2]
    scale = den + damp_ref[...]
    nw_re = wav_re + (cross_re - wav_re * den) / scale
    nw_im = wav_im + (cross_im - wav_im * den) / scale
    nw[0:1] = nw_re
    nw[1:2] = nw_im
    for b in range(lines):
        ins[b].wait()
        wg_re, wg_im = wg[0, b], wg[1, b]
        out_re = wd[0, b] - (nw_re * wg_re - nw_im * wg_im)
        out_im = wd[1, b] - (nw_re * wg_im + nw_im * wg_re)
        buf[b, 0] = out_re.reshape(shots, rb, f).astype(BF16)
        buf[b, 1] = out_im.reshape(shots, rb, f).astype(BF16)
        if b == 0:
            last = pltpu.make_async_copy(nw, nw_ref, nsem)
            last.start()
        else:
            outs[b - 1].start()
    outs[-1].start()
    for c in outs:
        c.wait()
    last.wait()


def swapped(x, axis, bit):
    size = lax.axis_size(axis)
    return lax.ppermute(x, axis, [(i, i ^ bit) for i in range(size)])


def sent_to_all(array, axis):
    size = lax.axis_size(axis)
    return lax.all_to_all(
        jnp.broadcast_to(array[None], (size, *array.shape)), axis, 0, 0, tiled=True
    )


def update(modeled, observed, mask, shot_order, line_of_slot, coupling, wavelet, damping):
    _, shots, lines, rb, f = modeled.shape
    slots = lax.axis_size(SHOT)
    held = observed.shape[2]
    pieces = lax.axis_size(RCV)
    rows = shots * rb
    traces = lines * rows
    flops = 8 * traces * f * f
    me = lax.axis_index(SHOT).astype(jnp.int32).reshape(1)

    own_spread = call(
        k_spread, jax.ShapeDtypeStruct((pieces, 2 * held, rb, f), BF16), [ANY], HBM,
        limit=BIG,
        scratch=[
            pltpu.VMEM((pieces, 2 * held, rb, f), BF16),
            pltpu.SemaphoreType.DMA((CHUNKS, 2 * held)),
            pltpu.SemaphoreType.DMA((CHUNKS,)),
        ],
    )(observed.reshape(2 * held, pieces, rb, f))
    own_natural = lax.all_to_all(own_spread, RCV, 0, 0, tiled=True)

    piece = jax.ShapeDtypeStruct((2, rows, f), BF16)
    live, *masked = call(
        k_mask, (jax.ShapeDtypeStruct((slots, rows, 128), F32), *[piece] * slots),
        [SM, SM, VM, VM],
    )(me, line_of_slot, modeled, mask)
    wide = jax.ShapeDtypeStruct((2, slots, rows, f), F32)
    dma = pltpu.SemaphoreType.DMA
    coup = pltpu.VMEM(coupling.shape, BF16)
    x_block = pltpu.VMEM((2, traces, f), BF16)
    b_block = pltpu.VMEM((2, 2 * f, f), BF16)
    w_block = pltpu.VMEM(wide.shape, F32)
    window_scratch = [coup, x_block, b_block, w_block, dma, dma((slots,)), dma((2,))]
    arrived = {0: masked[0]}
    for b in SWAPS:
        arrived[b] = swapped(masked[b], SHOT, b)
    wg_here = call(
        k_window, wide, [ANY] * (slots + 1), HBM, flops=flops,
        scratch=window_scratch, limit=WIN,
    )(*masked, coupling)
    own_group = call(
        k_group, jax.ShapeDtypeStruct((slots, 2, rows, f), BF16), [SM, VM], HBM,
        scratch=[pltpu.VMEM((slots, 2, rows, f), BF16), dma((slots,))], limit=GRP,
    )(shot_order, own_natural.reshape(pieces, held, 2, rb, f))
    own_here = lax.all_to_all(own_group, SHOT, 0, 0, tiled=True)
    sums = call(
        k_cross, jax.ShapeDtypeStruct((3, f), F32), [SM, SM, VM, VM] + [ANY] * slots,
        scratch=[x_block, x_block, b_block, dma((slots,))],
        limit=CRS, flops=2 * flops,
    )(me, shot_order, own_natural.reshape(pieces, held, 2, rb, f), coupling, *[arrived[b] for b in range(slots)])
    sums = sums.reshape(3 * f // 128, 128)
    for axis in ("c", "zl"):
        sums = sums + swapped(sums, axis, 1)
    others = {}
    for bit in (2, 1, 3):
        others[bit] = swapped(sums, ("zh", "zm"), bit)
    sums = (sums + others[1]) + (others[2] + others[3])
    parts = sent_to_all(sums.reshape(1, 3 * f), REST)
    wd_here = call(
        k_window_own, wide, [SM, ANY, ANY, ANY], HBM, flops=flops, limit=MID,
        scratch=[
            pltpu.VMEM(own_here.shape, BF16), pltpu.VMEM(live.shape, F32), coup, x_block, b_block,
            w_block, dma((3,)), dma((2,)),
        ],
    )(me, own_here, live, coupling)

    new_wavelet, residual = call(
        k_final,
        (jax.ShapeDtypeStruct((2, f), F32), jax.ShapeDtypeStruct(modeled.shape, BF16)),
        [SM, SM, VM, HBM, VM, VM, VM], [HBM, HBM],
        scratch=[
            w_block, pltpu.VMEM((slots, 2, shots, rb, f), BF16), pltpu.VMEM((2, f), F32),
            dma((slots,)), dma((slots,)), dma,
        ],
        limit=FIN,
    )(me, line_of_slot, wd_here, wg_here, parts, wavelet, damping.reshape(1, f))
    return new_wavelet, residual


def solution(mesh):
    fine = Mesh(mesh.devices.reshape((2,) * 8), SHOT + RCV)
    placed = (
        P(None, SHOT, None, RCV, None),
        P(None, SHOT, RCV, None, None),
        P(SHOT, None, RCV),
        P(),
        P(),
        P(),
        P(),
        P(),
    )
    return jax.shard_map(
        update,
        mesh=fine,
        in_specs=placed,
        out_specs=(P(), P(None, SHOT, None, RCV, None)),
        check_vma=False,
    )
```

```python
import jax
import jax.numpy as jnp
from jax import lax
from jax.experimental import pallas as pl
from jax.experimental.pallas import tpu as pltpu
from jax.sharding import Mesh, PartitionSpec as P

F32 = jnp.float32
BF16 = jnp.bfloat16
SHOT = ("xh", "yh", "yl")
RCV = ("xl", "zh", "zm", "zl", "c")
REST = ("xh", "yh", "yl", "xl")
PILE = ("zh", "zm", "zl", "c")
SWAPS = (4, 5, 6, 7, 1, 2, 3)

VM = pl.BlockSpec(memory_space=pltpu.VMEM)
SM = pl.BlockSpec(memory_space=pltpu.SMEM)
ANY = pl.BlockSpec(memory_space=pl.ANY)
HBM = pl.BlockSpec(memory_space=pltpu.HBM)


def call(body, outs, in_specs, out_specs=None, scratch=(), limit=12 << 20, flops=0, nbytes=1 << 20):
    many = isinstance(outs, (tuple, list))
    return pl.pallas_call(
        body,
        out_shape=outs,
        in_specs=in_specs,
        out_specs=out_specs if out_specs is not None else ([VM] * len(outs) if many else VM),
        scratch_shapes=list(scratch),
        compiler_params=pltpu.CompilerParams(vmem_limit_bytes=limit),
        cost_estimate=pl.CostEstimate(flops=flops, bytes_accessed=nbytes, transcendentals=0),
    )


CHUNKS = 4
BIG = 62 << 20
WIN = 61 << 20
CRS = 50 << 20
GRP = 51 << 20
FIN = 50 << 20


def k_spread(obs_ref, out_ref, buf, sem_in, sem_out):
    parts, pieces = obs_ref.shape[:2]
    held = parts // 2
    step = pieces // CHUNKS
    ins, outs = [], []
    for q in range(CHUNKS):
        rows = pl.ds(q * step, step)
        for i in range(parts):
            to = i % held * 2 + i // held
            ins.append(pltpu.make_async_copy(obs_ref.at[i, rows], buf.at[rows, to], sem_in.at[q, i]))
        outs.append(pltpu.make_async_copy(buf.at[rows], out_ref.at[rows], sem_out.at[q]))
    for c in ins:
        c.start()
    for q in range(CHUNKS):
        for i in range(parts):
            ins[q * parts + i].wait()
        outs[q].start()
    for c in outs:
        c.wait()


def couple(c_ref, b_ref):
    f = c_ref.shape[1]
    re, im = c_ref[0], c_ref[1]
    b_ref[0, :f] = re
    b_ref[0, f:] = -im
    b_ref[1, :f] = im
    b_ref[1, f:] = re


def k_mask(me_ref, slot_ref, mod_ref, mask_ref, live_ref, *out_refs):
    me = me_ref[0]
    shots, rb = mod_ref.shape[1], mod_ref.shape[3]
    f = mod_ref.shape[4]
    eye = lax.broadcasted_iota(jnp.int32, (rb, rb), 0) == lax.broadcasted_iota(jnp.int32, (rb, rb), 1)
    for b, out_ref in enumerate(out_refs):
        line = slot_ref[lax.bitwise_xor(me, b)]
        for s in range(shots):
            row = mask_ref[s, pl.ds(line, 1)].astype(F32)
            column = jnp.where(eye, row, 0.0).sum(axis=1, keepdims=True)
            rows = pl.ds(s * rb, rb)
            live_ref[b, rows] = jnp.broadcast_to(column, (rb, 128))
            live = jnp.broadcast_to(column, (rb, f)) > 0.5
            for c in range(2):
                x = mod_ref[c, s, line].astype(F32)
                out_ref[c, rows] = jnp.where(live, x, 0.0).astype(BF16)


def window(x_ref, b_ref, d):
    x = jnp.concatenate([x_ref[0], x_ref[1]], axis=1)
    return jnp.dot(x, b_ref[d], preferred_element_type=F32)


def window_out(x_ref, b_ref, out_ref, buf, sem):
    copies = []
    for d in range(2):
        buf[d] = window(x_ref, b_ref, d).reshape(buf.shape[1:])
        copies.append(pltpu.make_async_copy(buf.at[d], out_ref.at[d], sem.at[d]))
        if d:
            copies[d - 1].start()
    copies[-1].start()
    for c in copies:
        c.wait()


def k_window(*refs):
    xs, c_ref, (out_ref, coup, x_ref, b_ref, buf, csem, isem, sem) = refs[:-9], refs[-9], refs[-8:]
    rows = xs[0].shape[1]
    first = pltpu.make_async_copy(c_ref, coup, csem)
    first.start()
    ins = [
        pltpu.make_async_copy(x, x_ref.at[:, pl.ds(b * rows, rows)], isem.at[b])
        for b, x in enumerate(xs)
    ]
    for c in ins:
        c.start()
    first.wait()
    couple(coup, b_ref)
    for c in ins:
        c.wait()
    window_out(x_ref, b_ref, out_ref, buf, sem)


def fold(x):
    return x.reshape(x.shape[0] // 8, 8, x.shape[1]).sum(axis=0).sum(axis=0, keepdims=True)


def k_group(me_ref, order_ref, own_ref, send_ref, keep_ref, buf, sem):
    me = me_ref[0]
    half, _, rows, _ = send_ref.shape
    rb = own_ref.shape[3]
    size = rows // rb
    copies = [pltpu.make_async_copy(buf.at[d], send_ref.at[d], sem.at[d]) for d in range(half)]
    for first, to in ((half, buf), (0, keep_ref)):
        for d in range(half):
            g = lax.bitwise_xor(me, first + d)
            for s in range(size):
                n = order_ref[g * size + s]
                j = lax.shift_right_logical(n, 1)
                h = lax.bitwise_and(n, 1)
                for c in range(2):
                    to[d, c, s * rb : (s + 1) * rb] = own_ref[j, h, c]
            if first and d:
                copies[d - 1].start()
        if first:
            copies[-1].start()
    for c in copies:
        c.wait()


def k_pair(keep_ref, came_ref, *refs):
    out_refs, sem = refs[:-1], refs[-1]
    copies = [
        pltpu.make_async_copy(src.at[d], out_ref.at[i], sem.at[i, d])
        for i, src in ((1, came_ref), (0, keep_ref))
        for d, out_ref in enumerate(out_refs)
    ]
    for c in copies:
        c.start()
    for c in copies:
        c.wait()


def k_cross(me_ref, order_ref, own_ref, c_ref, *refs):
    mods, (sum_ref, x_ref, m_ref, b_ref, sem) = refs[:-5], refs[-5:]
    me = me_ref[0]
    groups = len(mods)
    rows, f = mods[0].shape[1:]
    rb = own_ref.shape[3]
    size = rows // rb
    copies = [
        pltpu.make_async_copy(mods[b], m_ref.at[:, pl.ds(b * rows, rows)], sem.at[b])
        for b in range(groups)
    ]
    for c in copies:
        c.start()

    def couple_rows(i, carry):
        block = f // 4
        upper, lower = pl.ds(pl.multiple_of(i * block, block), block), pl.ds(pl.multiple_of(f + i * block, block), block)
        re, im = c_ref[0, upper], c_ref[1, upper]
        b_ref[0, upper] = re
        b_ref[0, lower] = -im
        b_ref[1, upper] = im
        b_ref[1, lower] = re
        return carry

    lax.fori_loop(0, 4, couple_rows, 0)
    for b in range(groups):
        g = lax.bitwise_xor(me, b)
        for s in range(size):
            n = order_ref[g * size + s]
            j = lax.shift_right_logical(n, 1)
            h = lax.bitwise_and(n, 1)
            row = (b * size + s) * rb
            for c in range(2):
                x_ref[c, row : row + rb] = own_ref[j, h, c]
    wd_re, wd_im = window(x_ref, b_ref, 0), window(x_ref, b_ref, 1)
    for c in copies:
        c.wait()
    wg_re, wg_im = window(m_ref, b_ref, 0), window(m_ref, b_ref, 1)
    sum_ref[0:1] = fold(wg_re * wd_re + wg_im * wd_im)
    sum_ref[1:2] = fold(wg_re * wd_im - wg_im * wd_re)
    sum_ref[2:3] = fold(wg_re * wg_re + wg_im * wg_im)


def k_final(me_ref, slot_ref, *refs):
    pairs, refs = refs[:4], refs[4:]
    live_ref, c_ref, wg_ref, sums_ref, wav_ref, damp_ref, nw_ref, out_ref = refs[:8]
    own, live, coup, x_ref, b_ref, wd, wg, buf, nw, psem, lsem, sem, osem, nsem = refs[8:]
    me = me_ref[0]
    _, lines, rows, f = wg_ref.shape
    shots, rb = out_ref.shape[1], out_ref.shape[3]
    half = len(pairs)
    first = [pltpu.make_async_copy(c_ref, coup, lsem.at[0]), pltpu.make_async_copy(live_ref, live, lsem.at[1])]
    first += [pltpu.make_async_copy(p, own.at[d], psem.at[d]) for d, p in enumerate(pairs)]
    ins = [pltpu.make_async_copy(wg_ref.at[:, b], wg.at[:, b], sem.at[b]) for b in range(lines)]
    for c in first + ins:
        c.start()
    for c in first:
        c.wait()

    def couple_rows(i, carry):
        block = f // 4
        upper, lower = pl.ds(pl.multiple_of(i * block, block), block), pl.ds(pl.multiple_of(f + i * block, block), block)
        re, im = coup[0, upper], coup[1, upper]
        b_ref[0, upper] = re
        b_ref[0, lower] = -im
        b_ref[1, upper] = im
        b_ref[1, lower] = re
        return carry

    lax.fori_loop(0, 4, couple_rows, 0)
    for b in range(lines):
        alive = jnp.concatenate([live[b]] * (f // live.shape[2]), axis=1) > 0.5
        for c in range(2):
            x = own[b % half, b // half, c].astype(F32)
            x_ref[c, b * rows : (b + 1) * rows] = jnp.where(alive, x, 0.0).astype(BF16)
    for d in range(2):
        wd[d] = window(x_ref, b_ref, d).reshape(wd.shape[1:])
    outs = [
        pltpu.make_async_copy(
            buf.at[b], out_ref.at[:, :, slot_ref[lax.bitwise_xor(me, b)]], osem.at[b]
        )
        for b in range(lines)
    ]
    total = sums_ref[...].sum(axis=0)
    cross_re, cross_im, den = total[:, :f], total[:, f : 2 * f], total[:, 2 * f :]
    wav_re, wav_im = wav_ref[0:1], wav_ref[1:2]
    scale = den + damp_ref[...]
    nw_re = wav_re + (cross_re - wav_re * den) / scale
    nw_im = wav_im + (cross_im - wav_im * den) / scale
    nw[0:1] = nw_re
    nw[1:2] = nw_im
    for b in range(lines):
        ins[b].wait()
        wg_re, wg_im = wg[0, b], wg[1, b]
        out_re = wd[0, b] - (nw_re * wg_re - nw_im * wg_im)
        out_im = wd[1, b] - (nw_re * wg_im + nw_im * wg_re)
        buf[b, 0] = out_re.reshape(shots, rb, f).astype(BF16)
        buf[b, 1] = out_im.reshape(shots, rb, f).astype(BF16)
        if b == 0:
            last = pltpu.make_async_copy(nw, nw_ref, nsem)
            last.start()
        else:
            outs[b - 1].start()
    outs[-1].start()
    for c in outs:
        c.wait()
    last.wait()


def swapped(x, axis, bit):
    size = lax.axis_size(axis)
    return lax.ppermute(x, axis, [(i, i ^ bit) for i in range(size)])


def sent_to_all(array, axis):
    size = lax.axis_size(axis)
    return lax.all_to_all(
        jnp.broadcast_to(array[None], (size, *array.shape)), axis, 0, 0, tiled=True
    )


def update(modeled, observed, mask, shot_order, line_of_slot, coupling, wavelet, damping):
    _, shots, lines, rb, f = modeled.shape
    slots = lax.axis_size(SHOT)
    held = observed.shape[2]
    pieces = lax.axis_size(RCV)
    rows = shots * rb
    traces = lines * rows
    flops = 8 * traces * f * f
    me = lax.axis_index(SHOT).astype(jnp.int32).reshape(1)

    own_spread = call(
        k_spread, jax.ShapeDtypeStruct((pieces, 2 * held, rb, f), BF16), [ANY], HBM,
        limit=BIG,
        scratch=[
            pltpu.VMEM((pieces, 2 * held, rb, f), BF16),
            pltpu.SemaphoreType.DMA((CHUNKS, 2 * held)),
            pltpu.SemaphoreType.DMA((CHUNKS,)),
        ],
    )(observed.reshape(2 * held, pieces, rb, f))
    own_natural = lax.all_to_all(own_spread, RCV, 0, 0, tiled=True)

    piece = jax.ShapeDtypeStruct((2, rows, f), BF16)
    live, *masked = call(
        k_mask, (jax.ShapeDtypeStruct((slots, rows, 128), F32), *[piece] * slots),
        [SM, SM, VM, VM],
    )(me, line_of_slot, modeled, mask)
    wide = jax.ShapeDtypeStruct((2, slots, rows, f), F32)
    dma = pltpu.SemaphoreType.DMA
    coup = pltpu.VMEM(coupling.shape, BF16)
    x_block = pltpu.VMEM((2, traces, f), BF16)
    b_block = pltpu.VMEM((2, 2 * f, f), BF16)
    w_block = pltpu.VMEM(wide.shape, F32)
    window_scratch = [coup, x_block, b_block, w_block, dma, dma((slots,)), dma((2,))]
    arrived = {0: masked[0]}
    for b in SWAPS:
        arrived[b] = swapped(masked[b], SHOT, b)
    wg_here = call(
        k_window, wide, [ANY] * (slots + 1), HBM, flops=flops,
        scratch=window_scratch, limit=WIN,
    )(*masked, coupling)
    half = slots // 2
    quad = jax.ShapeDtypeStruct((half, 2, rows, f), BF16)
    own_send, own_keep = call(
        k_group, (quad, quad), [SM, SM, VM], [HBM, VM], limit=GRP,
        scratch=[pltpu.VMEM(quad.shape, BF16), dma((half,))],
    )(
        me, shot_order, own_natural.reshape(pieces, held, 2, rb, f)
    )
    own_came = swapped(own_send, "xh", 1)
    sums = call(
        k_cross, jax.ShapeDtypeStruct((3, f), F32), [SM, SM, VM, VM] + [ANY] * slots,
        scratch=[x_block, x_block, b_block, dma((slots,))],
        limit=CRS, flops=2 * flops,
    )(me, shot_order, own_natural.reshape(pieces, held, 2, rb, f), coupling, *[arrived[b] for b in range(slots)])
    part = sent_to_all(sums.reshape(1, 3 * f), PILE).sum(axis=0)
    couple_of = jax.ShapeDtypeStruct((2, 2, rows, f), BF16)
    pairs = call(k_pair, (couple_of,) * half, [ANY, ANY], scratch=[dma((2, half))])(own_keep, own_came)
    met = {0: pairs[0]}
    for b in (1, 3, 2):
        met[b] = swapped(pairs[b], ("yh", "yl"), b)
    parts = sent_to_all(part, REST)
    new_wavelet, residual = call(
        k_final,
        (jax.ShapeDtypeStruct((2, f), F32), jax.ShapeDtypeStruct(modeled.shape, BF16)),
        [SM, SM] + [ANY] * (half + 2) + [HBM, VM, VM, VM], [HBM, HBM],
        scratch=[
            pltpu.VMEM((half, 2, 2, rows, f), BF16), pltpu.VMEM(live.shape, F32), coup, x_block, b_block,
            w_block, w_block, pltpu.VMEM((slots, 2, shots, rb, f), BF16), pltpu.VMEM((2, f), F32),
            dma((half,)), dma((2,)), dma((slots,)), dma((slots,)), dma,
        ],
        limit=FIN, flops=flops,
    )(
        me, line_of_slot, *[met[d] for d in range(half)], live, coupling, wg_here,
        parts, wavelet, damping.reshape(1, f),
    )
    return new_wavelet, residual


def solution(mesh):
    fine = Mesh(mesh.devices.reshape((2,) * 8), SHOT + RCV)
    placed = (
        P(None, SHOT, None, RCV, None),
        P(None, SHOT, RCV, None, None),
        P(SHOT, None, RCV),
        P(),
        P(),
        P(),
        P(),
        P(),
    )
    return jax.shard_map(
        update,
        mesh=fine,
        in_specs=placed,
        out_specs=(P(), P(None, SHOT, None, RCV, None)),
        check_vma=False,
    )
```

```python
import jax
import jax.numpy as jnp
from jax import lax
from jax.experimental import pallas as pl
from jax.experimental.pallas import tpu as pltpu
from jax.sharding import Mesh, PartitionSpec as P

F32 = jnp.float32
BF16 = jnp.bfloat16
SHOT = ("xh", "yh", "yl")
RCV = ("xl", "zh", "zm", "zl", "c")
REST = ("xh", "yh", "yl", "xl")
PILE = ("zh", "zm", "zl", "c")
SWAPS = (4, 5, 6, 7, 1, 2, 3)

VM = pl.BlockSpec(memory_space=pltpu.VMEM)
SM = pl.BlockSpec(memory_space=pltpu.SMEM)
ANY = pl.BlockSpec(memory_space=pl.ANY)
HBM = pl.BlockSpec(memory_space=pltpu.HBM)


def call(body, outs, in_specs, out_specs=None, scratch=(), limit=12 << 20, flops=0, nbytes=1 << 20):
    many = isinstance(outs, (tuple, list))
    return pl.pallas_call(
        body,
        out_shape=outs,
        in_specs=in_specs,
        out_specs=out_specs if out_specs is not None else ([VM] * len(outs) if many else VM),
        scratch_shapes=list(scratch),
        compiler_params=pltpu.CompilerParams(vmem_limit_bytes=limit),
        cost_estimate=pl.CostEstimate(flops=flops, bytes_accessed=nbytes, transcendentals=0),
    )


CHUNKS = 4
BIG = 62 << 20
WIN = 61 << 20
CRS = 50 << 20
GRP = 51 << 20
FIN = 50 << 20


def k_spread(obs_ref, out_ref, buf, sem_in, sem_out):
    parts, pieces = obs_ref.shape[:2]
    held = parts // 2
    step = pieces // CHUNKS
    ins, outs = [], []
    for q in range(CHUNKS):
        rows = pl.ds(q * step, step)
        for i in range(parts):
            to = i % held * 2 + i // held
            ins.append(pltpu.make_async_copy(obs_ref.at[i, rows], buf.at[rows, to], sem_in.at[q, i]))
        outs.append(pltpu.make_async_copy(buf.at[rows], out_ref.at[rows], sem_out.at[q]))
    for c in ins:
        c.start()
    for q in range(CHUNKS):
        for i in range(parts):
            ins[q * parts + i].wait()
        outs[q].start()
    for c in outs:
        c.wait()


def couple(c_ref, b_ref):
    f = c_ref.shape[1]
    re, im = c_ref[0], c_ref[1]
    b_ref[0, :f] = re
    b_ref[0, f:] = -im
    b_ref[1, :f] = im
    b_ref[1, f:] = re


def k_mask(me_ref, slot_ref, mod_ref, mask_ref, live_ref, *out_refs):
    me = me_ref[0]
    shots, rb = mod_ref.shape[1], mod_ref.shape[3]
    f = mod_ref.shape[4]
    eye = lax.broadcasted_iota(jnp.int32, (rb, rb), 0) == lax.broadcasted_iota(jnp.int32, (rb, rb), 1)
    for b, out_ref in enumerate(out_refs):
        line = slot_ref[lax.bitwise_xor(me, b)]
        for s in range(shots):
            row = mask_ref[s, pl.ds(line, 1)].astype(F32)
            column = jnp.where(eye, row, 0.0).sum(axis=1, keepdims=True)
            rows = pl.ds(s * rb, rb)
            live_ref[b, rows] = jnp.broadcast_to(column, (rb, 128))
            live = jnp.broadcast_to(column, (rb, f)) > 0.5
            for c in range(2):
                x = mod_ref[c, s, line].astype(F32)
                out_ref[c, rows] = jnp.where(live, x, 0.0).astype(BF16)


def window(x_ref, b_ref, d):
    x = jnp.concatenate([x_ref[0], x_ref[1]], axis=1)
    return jnp.dot(x, b_ref[d], preferred_element_type=F32)


def window_out(x_ref, b_ref, out_ref, buf, sem):
    copies = []
    for d in range(2):
        buf[d] = window(x_ref, b_ref, d).reshape(buf.shape[1:])
        copies.append(pltpu.make_async_copy(buf.at[d], out_ref.at[d], sem.at[d]))
        if d:
            copies[d - 1].start()
    copies[-1].start()
    for c in copies:
        c.wait()


def k_window(*refs):
    xs, c_ref, (out_ref, coup, x_ref, b_ref, buf, csem, isem, sem) = refs[:-9], refs[-9], refs[-8:]
    rows = xs[0].shape[1]
    first = pltpu.make_async_copy(c_ref, coup, csem)
    first.start()
    ins = [
        pltpu.make_async_copy(x, x_ref.at[:, pl.ds(b * rows, rows)], isem.at[b])
        for b, x in enumerate(xs)
    ]
    for c in ins:
        c.start()
    first.wait()
    couple(coup, b_ref)
    for c in ins:
        c.wait()
    window_out(x_ref, b_ref, out_ref, buf, sem)


def fold(x):
    return x.reshape(x.shape[0] // 8, 8, x.shape[1]).sum(axis=0).sum(axis=0, keepdims=True)


def k_group(me_ref, order_ref, own_ref, send_ref, keep_ref):
    me = me_ref[0]
    half, _, rows, _ = send_ref.shape
    rb = own_ref.shape[3]
    size = rows // rb
    for first, out_ref in ((half, send_ref), (0, keep_ref)):
        for d in range(half):
            g = lax.bitwise_xor(me, first + d)
            for s in range(size):
                n = order_ref[g * size + s]
                j = lax.shift_right_logical(n, 1)
                h = lax.bitwise_and(n, 1)
                for c in range(2):
                    out_ref[d, c, s * rb : (s + 1) * rb] = own_ref[j, h, c]


def k_pair(keep_ref, came_ref, *out_refs):
    for d, out_ref in enumerate(out_refs):
        out_ref[0] = keep_ref[d]
        out_ref[1] = came_ref[d]


def k_cross(me_ref, order_ref, own_ref, c_ref, *refs):
    mods, (sum_ref, x_ref, m_ref, b_ref, sem) = refs[:-5], refs[-5:]
    me = me_ref[0]
    groups = len(mods)
    rows, f = mods[0].shape[1:]
    rb = own_ref.shape[3]
    size = rows // rb
    copies = [
        pltpu.make_async_copy(mods[b], m_ref.at[:, pl.ds(b * rows, rows)], sem.at[b])
        for b in range(groups)
    ]
    for c in copies:
        c.start()

    def couple_rows(i, carry):
        block = f // 4
        upper, lower = pl.ds(pl.multiple_of(i * block, block), block), pl.ds(pl.multiple_of(f + i * block, block), block)
        re, im = c_ref[0, upper], c_ref[1, upper]
        b_ref[0, upper] = re
        b_ref[0, lower] = -im
        b_ref[1, upper] = im
        b_ref[1, lower] = re
        return carry

    lax.fori_loop(0, 4, couple_rows, 0)
    for b in range(groups):
        g = lax.bitwise_xor(me, b)
        for s in range(size):
            n = order_ref[g * size + s]
            j = lax.shift_right_logical(n, 1)
            h = lax.bitwise_and(n, 1)
            row = (b * size + s) * rb
            for c in range(2):
                x_ref[c, row : row + rb] = own_ref[j, h, c]
    wd_re, wd_im = window(x_ref, b_ref, 0), window(x_ref, b_ref, 1)
    for c in copies:
        c.wait()
    wg_re, wg_im = window(m_ref, b_ref, 0), window(m_ref, b_ref, 1)
    sum_ref[0:1] = fold(wg_re * wd_re + wg_im * wd_im)
    sum_ref[1:2] = fold(wg_re * wd_im - wg_im * wd_re)
    sum_ref[2:3] = fold(wg_re * wg_re + wg_im * wg_im)


def k_final(me_ref, slot_ref, *refs):
    pairs, refs = refs[:4], refs[4:]
    live_ref, c_ref, wg_ref, sums_ref, wav_ref, damp_ref, nw_ref, out_ref = refs[:8]
    own, live, coup, x_ref, b_ref, wd, wg, buf, nw, psem, lsem, sem, osem, nsem = refs[8:]
    me = me_ref[0]
    _, lines, rows, f = wg_ref.shape
    shots, rb = out_ref.shape[1], out_ref.shape[3]
    half = len(pairs)
    first = [pltpu.make_async_copy(c_ref, coup, lsem.at[0]), pltpu.make_async_copy(live_ref, live, lsem.at[1])]
    first += [pltpu.make_async_copy(p, own.at[d], psem.at[d]) for d, p in enumerate(pairs)]
    ins = [pltpu.make_async_copy(wg_ref.at[:, b], wg.at[:, b], sem.at[b]) for b in range(lines)]
    for c in first + ins:
        c.start()
    for c in first:
        c.wait()

    def couple_rows(i, carry):
        block = f // 4
        upper, lower = pl.ds(pl.multiple_of(i * block, block), block), pl.ds(pl.multiple_of(f + i * block, block), block)
        re, im = coup[0, upper], coup[1, upper]
        b_ref[0, upper] = re
        b_ref[0, lower] = -im
        b_ref[1, upper] = im
        b_ref[1, lower] = re
        return carry

    lax.fori_loop(0, 4, couple_rows, 0)
    for b in range(lines):
        alive = jnp.concatenate([live[b]] * (f // live.shape[2]), axis=1) > 0.5
        for c in range(2):
            x = own[b % half, b // half, c].astype(F32)
            x_ref[c, b * rows : (b + 1) * rows] = jnp.where(alive, x, 0.0).astype(BF16)
    for d in range(2):
        wd[d] = window(x_ref, b_ref, d).reshape(wd.shape[1:])
    outs = [
        pltpu.make_async_copy(
            buf.at[b], out_ref.at[:, :, slot_ref[lax.bitwise_xor(me, b)]], osem.at[b]
        )
        for b in range(lines)
    ]
    total = sums_ref[...].sum(axis=0)
    cross_re, cross_im, den = total[:, :f], total[:, f : 2 * f], total[:, 2 * f :]
    wav_re, wav_im = wav_ref[0:1], wav_ref[1:2]
    scale = den + damp_ref[...]
    nw_re = wav_re + (cross_re - wav_re * den) / scale
    nw_im = wav_im + (cross_im - wav_im * den) / scale
    nw[0:1] = nw_re
    nw[1:2] = nw_im
    for b in range(lines):
        ins[b].wait()
        wg_re, wg_im = wg[0, b], wg[1, b]
        out_re = wd[0, b] - (nw_re * wg_re - nw_im * wg_im)
        out_im = wd[1, b] - (nw_re * wg_im + nw_im * wg_re)
        buf[b, 0] = out_re.reshape(shots, rb, f).astype(BF16)
        buf[b, 1] = out_im.reshape(shots, rb, f).astype(BF16)
        if b == 0:
            last = pltpu.make_async_copy(nw, nw_ref, nsem)
            last.start()
        else:
            outs[b - 1].start()
    outs[-1].start()
    for c in outs:
        c.wait()
    last.wait()


def swapped(x, axis, bit):
    size = lax.axis_size(axis)
    return lax.ppermute(x, axis, [(i, i ^ bit) for i in range(size)])


def sent_to_all(array, axis):
    size = lax.axis_size(axis)
    return lax.all_to_all(
        jnp.broadcast_to(array[None], (size, *array.shape)), axis, 0, 0, tiled=True
    )


def update(modeled, observed, mask, shot_order, line_of_slot, coupling, wavelet, damping):
    _, shots, lines, rb, f = modeled.shape
    slots = lax.axis_size(SHOT)
    held = observed.shape[2]
    pieces = lax.axis_size(RCV)
    rows = shots * rb
    traces = lines * rows
    flops = 8 * traces * f * f
    me = lax.axis_index(SHOT).astype(jnp.int32).reshape(1)

    own_spread = call(
        k_spread, jax.ShapeDtypeStruct((pieces, 2 * held, rb, f), BF16), [ANY], HBM,
        limit=BIG,
        scratch=[
            pltpu.VMEM((pieces, 2 * held, rb, f), BF16),
            pltpu.SemaphoreType.DMA((CHUNKS, 2 * held)),
            pltpu.SemaphoreType.DMA((CHUNKS,)),
        ],
    )(observed.reshape(2 * held, pieces, rb, f))
    own_natural = lax.all_to_all(own_spread, RCV, 0, 0, tiled=True)

    piece = jax.ShapeDtypeStruct((2, rows, f), BF16)
    live, *masked = call(
        k_mask, (jax.ShapeDtypeStruct((slots, rows, 128), F32), *[piece] * slots),
        [SM, SM, VM, VM],
    )(me, line_of_slot, modeled, mask)
    wide = jax.ShapeDtypeStruct((2, slots, rows, f), F32)
    dma = pltpu.SemaphoreType.DMA
    coup = pltpu.VMEM(coupling.shape, BF16)
    x_block = pltpu.VMEM((2, traces, f), BF16)
    b_block = pltpu.VMEM((2, 2 * f, f), BF16)
    w_block = pltpu.VMEM(wide.shape, F32)
    window_scratch = [coup, x_block, b_block, w_block, dma, dma((slots,)), dma((2,))]
    arrived = {0: masked[0]}
    for b in SWAPS:
        arrived[b] = swapped(masked[b], SHOT, b)
    wg_here = call(
        k_window, wide, [ANY] * (slots + 1), HBM, flops=flops,
        scratch=window_scratch, limit=WIN,
    )(*masked, coupling)
    half = slots // 2
    quad = jax.ShapeDtypeStruct((half, 2, rows, f), BF16)
    own_send, own_keep = call(k_group, (quad, quad), [SM, SM, VM], limit=GRP)(
        me, shot_order, own_natural.reshape(pieces, held, 2, rb, f)
    )
    own_came = swapped(own_send, "xh", 1)
    sums = call(
        k_cross, jax.ShapeDtypeStruct((3, f), F32), [SM, SM, VM, VM] + [ANY] * slots,
        scratch=[x_block, x_block, b_block, dma((slots,))],
        limit=CRS, flops=2 * flops,
    )(me, shot_order, own_natural.reshape(pieces, held, 2, rb, f), coupling, *[arrived[b] for b in range(slots)])
    part = sent_to_all(sums.reshape(1, 3 * f), PILE).sum(axis=0)
    couple_of = jax.ShapeDtypeStruct((2, 2, rows, f), BF16)
    pairs = call(k_pair, (couple_of,) * half, [VM, VM])(own_keep, own_came)
    met = {0: pairs[0]}
    for b in (2, 1, 3):
        met[b] = swapped(pairs[b], ("yh", "yl"), b)
    parts = sent_to_all(part, REST)
    new_wavelet, residual = call(
        k_final,
        (jax.ShapeDtypeStruct((2, f), F32), jax.ShapeDtypeStruct(modeled.shape, BF16)),
        [SM, SM] + [ANY] * (half + 2) + [HBM, VM, VM, VM], [HBM, HBM],
        scratch=[
            pltpu.VMEM((half, 2, 2, rows, f), BF16), pltpu.VMEM(live.shape, F32), coup, x_block, b_block,
            w_block, w_block, pltpu.VMEM((slots, 2, shots, rb, f), BF16), pltpu.VMEM((2, f), F32),
            dma((half,)), dma((2,)), dma((slots,)), dma((slots,)), dma,
        ],
        limit=FIN, flops=flops,
    )(
        me, line_of_slot, *[met[d] for d in range(half)], live, coupling, wg_here,
        parts, wavelet, damping.reshape(1, f),
    )
    return new_wavelet, residual


def solution(mesh):
    fine = Mesh(mesh.devices.reshape((2,) * 8), SHOT + RCV)
    placed = (
        P(None, SHOT, None, RCV, None),
        P(None, SHOT, RCV, None, None),
        P(SHOT, None, RCV),
        P(),
        P(),
        P(),
        P(),
        P(),
    )
    return jax.shard_map(
        update,
        mesh=fine,
        in_specs=placed,
        out_specs=(P(), P(None, SHOT, None, RCV, None)),
        check_vma=False,
    )
```
